128 devices in a mesh: dp: 16 (over x_hi, z, core), tensor: 8 (over x_lo, y).
Axes of the slice: x: 4 (x_hi: 2, x_lo: 2; x = x_hi * 2 + x_lo), y: 4, z: 4, core: 2. Of those that a mesh axis runs over, the one named last changes fastest.
Arguments:
- tokens: bfloat16 [20480, 4096], P(('dp', 'tensor')), parts along dimension 0, may hold values from -6 to 6
- norm_gain: bfloat16 [4096], replicated, may hold values from 0.099609375 to 1.8984375
- query_weight: bfloat16 [4096, 8192], P(None, 'tensor'), may hold values from -0.09375 to 0.09375
- key_weight: bfloat16 [4096, 1024], P(None, 'tensor'), may hold values from -0.09375 to 0.09375
- value_weight: bfloat16 [4096, 1024], P(None, 'tensor'), may hold values from -0.09375 to 0.09375
- out_weight: bfloat16 [8192, 4096], P('tensor'), may hold values from -0.0625 to 0.0625
- past_cache: bfloat16 [2048, 64, 2, 1024], P('dp', None, None, 'tensor'), parts along dimension 0, may hold values from -320 to 320
- exponents: int32 [20480, 32], P('dp'), parts along dimension 0, may hold values from -11 to -7
Outputs:
- mixed: bfloat16 [20480, 4096], P(('dp', 'tensor')), parts along dimension 0
The draws below stay inside these ranges and needn't reach their ends.
There are 16 independent parts, one for each index of `dp`. The reference program is written for one: setup_inputs(seed, part) draws one part's arguments, and reference() takes and returns one part's arrays. A program takes and returns all parts, laid end to end along the dimension named above; an argument that names none is the same for every part. Nothing has to cross between parts.
All inputs are finite; a program needn't handle non-finite values.
Results may differ from the reference program's by a relative error of at most 0.012.
The reference program's roundings to bfloat16 on the way count: a program that leaves them out, or rounds other values in their place, can miss the bound.
Values may be sent and summed in bfloat16 or wider, within the bound.
A program may use at most 192 MiB of HBM per device.

```python
import jax
import jax.numpy as jnp
from jax import lax

D = 4096
QH = 64
KVH = 8
HD = 128
SEQS = 128
NEW = 10
CACHE = 64
QG = 128
ROWS = 1280
N_TENSOR = 8


def draw_past_cache(key, part):
    key_base = jax.random.fold_in(key, 11)
    shape_full = (SEQS, CACHE, 2, KVH * HD)
    values_out = jnp.clip(jax.random.normal(key_base, shape_full, jnp.float32), -4.0, 4.0)
    return values_out.astype(jnp.bfloat16)


def with_ends(array, key, least, top_value):
    longest = array.shape.index(max(array.shape))
    spots = []
    for shift in (0, 1):
        where = [jax.random.randint(jax.random.fold_in(key, axis), (), 0, length) for axis, length in enumerate(array.shape)]
        where[longest] = (where[longest] + shift) % array.shape[longest]
        spots.append(tuple(where))
    return array.at[spots[0]].set(least).at[spots[1]].set(top_value)


def block_scale(rng, dims, pieces, smallest, high):
    def one(dim, blocks):
        draws = jax.random.uniform(jax.random.fold_in(jax.random.fold_in(rng, 6), dim), (blocks,), jnp.float32, smallest / len(pieces), high / len(pieces))
        return jnp.repeat(jnp.exp(draws), dims[dim] // blocks).reshape((-1,) + (1,) * (len(dims) - dim - 1))

    gain = one(*pieces[0])
    for cut in pieces[1:]:
        gain = gain * one(*cut)
    return gain


def scatter_about(own_key, shape, width, limit, pieces=(), kind=jnp.bfloat16):
    gain = block_scale(own_key, shape, pieces, -0.22, 0.18) if pieces else 1.0
    result = jax.random.normal(own_key, shape, jnp.float32) * width * gain
    return jnp.minimum(jnp.maximum(result, -limit), limit).astype(kind)


def setup_inputs(seed: int = 0, part: int = 0) -> dict:
    streams_of = jax.random.split(jax.random.key(seed), 9)
    own_keys = jax.random.split(jax.random.fold_in(streams_of[8], part), 9)
    return {
        "tokens": scatter_about(own_keys[0], (ROWS, D), 1.0, 6.0, ((0, 8),)),
        "norm_gain": jnp.clip(1.0 + 0.18 * jax.random.normal(streams_of[1], (D,), jnp.float32), 0.099609375, 1.8984375).astype(jnp.bfloat16),
        "query_weight": scatter_about(streams_of[2], (D, QH * HD), D ** -0.5, 0.09375, ((1, 8),)),
        "key_weight": scatter_about(streams_of[3], (D, KVH * HD), D ** -0.5, 0.09375, ((1, 8),)),
        "value_weight": scatter_about(streams_of[4], (D, KVH * HD), D ** -0.5, 0.09375, ((1, 8),)),
        "out_weight": scatter_about(streams_of[5], (QH * HD, D), (QH * HD) ** -0.5, 0.0625, ((0, 8),)),
        "past_cache": draw_past_cache(jax.random.fold_in(jax.random.fold_in(streams_of[8], part), 71), part),
        "exponents": with_ends(jax.random.randint(own_keys[7], (ROWS, D // QG), -11, -6), jax.random.fold_in(own_keys[7], 1), -11, (-6) - 1).astype(jnp.int32),
    }


epsilon = 1e-05
theta_base = 500000.0

def rotate(matrix, heads):
    row_count = matrix.shape[0]
    half_dim = HD // 2
    positions = (jnp.arange(row_count, dtype=jnp.int32) % NEW + CACHE).astype(jnp.float32)
    frequency = theta_base ** (-(jnp.arange(half_dim, dtype=jnp.float32) * 2.0) / HD)
    angles = positions[:, None] * frequency[None, :]
    cosine = jnp.cos(angles)[:, None, :]
    sine_part = jnp.sin(angles)[:, None, :]
    shaped = matrix.reshape(row_count, heads, 2, half_dim)
    first = shaped[:, :, 0]
    second = shaped[:, :, 1]
    turned = jnp.stack([first * cosine - second * sine_part, second * cosine + first * sine_part], 2)
    return turned.reshape(row_count, heads * HD)

def attention(query, key_new, value_new, past_cache, kv_heads):
    row_count = query.shape[0]
    seq_count = row_count // NEW
    group_size = query.shape[1] // (kv_heads * HD)
    cache_len = past_cache.shape[1]
    query_heads = query.astype(jnp.float32).reshape(seq_count, NEW, kv_heads, group_size, HD)
    new_keys = key_new.astype(jnp.float32).reshape(seq_count, NEW, kv_heads, HD)
    new_values = value_new.astype(jnp.float32).reshape(seq_count, NEW, kv_heads, HD)
    cache_keys = past_cache[:, :, 0].astype(jnp.float32).reshape(seq_count, cache_len, kv_heads, HD)
    cache_values = past_cache[:, :, 1].astype(jnp.float32).reshape(seq_count, cache_len, kv_heads, HD)
    inv_root = 1.0 / HD ** 0.5
    cache_scores = jnp.einsum('stkgd,sckd->skgtc', query_heads, cache_keys) * inv_root
    new_scores = jnp.einsum('stkgd,sukd->skgtu', query_heads, new_keys) * inv_root
    causal = jnp.arange(NEW)[:, None] >= jnp.arange(NEW)[None, :]
    new_scores = jnp.where(causal, new_scores, -1e+30)
    row_max = jnp.maximum(cache_scores.max(-1), new_scores.max(-1))[..., None]
    cache_probs = jnp.exp(cache_scores - row_max)
    new_probs = jnp.exp(new_scores - row_max)
    denominator = (cache_probs.sum(-1) + new_probs.sum(-1))[..., None]
    cache_weights = (cache_probs / denominator).astype(jnp.bfloat16).astype(jnp.float32)
    new_weights = (new_probs / denominator).astype(jnp.bfloat16).astype(jnp.float32)
    combined = jnp.einsum('skgtc,sckd->stkgd', cache_weights, cache_values)
    combined = combined + jnp.einsum('skgtu,sukd->stkgd', new_weights, new_values)
    return combined.reshape(row_count, kv_heads * group_size * HD).astype(jnp.bfloat16)

def reference(tokens, norm_gain, query_weight, key_weight, value_weight, out_weight, past_cache, exponents):
    floats = tokens.astype(jnp.float32)
    normed = floats * lax.rsqrt(lax.optimization_barrier(jnp.mean(floats * floats, axis=-1, keepdims=True)) + epsilon)
    normed = (normed * norm_gain.astype(jnp.float32)).astype(jnp.bfloat16)
    query = rotate(jnp.dot(normed, query_weight, preferred_element_type=jnp.float32), QH).astype(jnp.bfloat16)
    key_new = rotate(jnp.dot(normed, key_weight, preferred_element_type=jnp.float32), KVH).astype(jnp.bfloat16)
    value_new = jnp.dot(normed, value_weight, preferred_element_type=jnp.float32).astype(jnp.bfloat16)
    attended = attention(query, key_new, value_new, past_cache, KVH)
    row_count = tokens.shape[0]
    groups = D // QG
    shrink = jnp.exp2(-exponents.astype(jnp.float32))[..., None]
    head_cols = QH * HD // N_TENSOR
    summed = jnp.zeros((row_count, groups, QG), jnp.float32)
    for rank in range(N_TENSOR):
        partial_value = jnp.dot(attended[:, rank * head_cols:(rank + 1) * head_cols], out_weight[rank * head_cols:(rank + 1) * head_cols], preferred_element_type=jnp.float32)
        scaled = jnp.clip(partial_value.reshape(row_count, groups, QG) * shrink, -127.0, 127.0)
        summed = summed + lax.optimization_barrier(scaled.astype(jnp.bfloat16)).astype(jnp.float32)
    restore = jnp.exp2(exponents.astype(jnp.float32))[..., None]
    layer_out = floats + (summed * restore).reshape(row_count, D)
    return layer_out.astype(jnp.bfloat16)
```

```python
import functools

import jax
import jax.numpy as jnp
import numpy as np
from jax import lax
from jax.experimental import pallas as pl
from jax.experimental.pallas import tpu as pltpu
from jax.sharding import PartitionSpec as P

HD = 128
NEW = 10
CACHE = 64
D = 4096
HEADS = 8
QC = 1024
SEQ_BLOCK = 16
ROWS_B = 160
PADDED = 256
CH = 1024
NQ = 4
EPS = 1e-05
THETA = 500000.0
MESH = pl.DeviceIdType.MESH
F32 = jnp.float32
BF16 = jnp.bfloat16

SLOTS = ((0, 0), (0, 3), (0, 1), (1, 0), (0, 2), (1, 2), (1, 3), (1, 1))
DX_BITS = sum(dx << j for j, (dx, _) in enumerate(SLOTS))
DY_BITS = sum(dy << (2 * j) for j, (_, dy) in enumerate(SLOTS))

UP, DOWN, ACROSS = "up", "down", "across"
GATHER = {
    "own_up": (UP, "x", 0, "x", 1, (0, 1, 2, 3)),
    "own_down": (DOWN, "x", 0, "x", 2, (2, 3, 0, 1)),
    "own_across": (ACROSS, "x", 0, "x", 3, (0, 1, 2, 3)),
    "far_up": (UP, "x", 1, "x", 4, (0, 1)),
    "far_down": (DOWN, "x", 2, "x", 4, (2, 3)),
    "far_across": (ACROSS, "x", 4, "x", 5, (0, 2, 1, 3)),
    "side_up": (UP, "x", 3, "x", 6, (0, 1, 2, 3)),
    "side_down": (DOWN, "x", 3, "x", 7, (0, 1, 2, 3)),
}
R_FAR, R_HALF, R_SIDE_P, R_SIDE_M, R_P, R_M, R_X = range(7)
SCATTER = {
    "r_far": (ACROSS, "p", 5, "r", R_FAR, (0, 2, 1, 3)),
    "r_half_down": (DOWN, "p", 4, "r", R_HALF, (0, 1)),
    "r_half_up": (UP, "p", 4, "r", R_HALF, (2, 3)),
    "r_near_down": (DOWN, "p", 1, "r", R_P, (2, 3, 0, 1)),
    "r_near_up": (UP, "p", 2, "r", R_M, (0, 1, 2, 3)),
    "r_side_down": (DOWN, "p", 6, "r", R_SIDE_P, (0, 1, 2, 3)),
    "r_side_up": (UP, "p", 7, "r", R_SIDE_M, (0, 1, 2, 3)),
    "r_across": (ACROSS, "p", 3, "r", R_X, (0, 1, 2, 3)),
}
ROUTES = {**GATHER, **SCATTER}
ROUTE_ID = {name: i for i, name in enumerate(ROUTES)}


def body(
    tokens_hbm, gain_ref, wq_hbm, wk_hbm, wv_hbm, wo_hbm, kv_hbm, exps_ref, cos_ref, sin_ref,
    pad_ref, unpad_ref, out_hbm,
    xg, pb, rb, w_in, w_out, kv, xn, qp, ap, ab, obuf,
    load_sem, send_sem, recv_sem, out_sem,
):
    me = lax.axis_index("tensor")
    mx, my = me // 4, me % 4
    targets = {
        UP: mx * 4 + (my + 1) % 4,
        DOWN: mx * 4 + (my + 3) % 4,
        ACROSS: (1 - mx) * 4 + my,
    }
    buffers = {"x": xg, "p": pb, "r": rb}

    def cols(q):
        return pl.ds(q * CH, CH)

    def route(name, q):
        link, sbuf, sslot, dbuf, dslot, _ = ROUTES[name]
        k = ROUTE_ID[name] * NQ + q
        return pltpu.make_async_remote_copy(
            src_ref=buffers[sbuf].at[sslot, :, cols(q)],
            dst_ref=buffers[dbuf].at[dslot, :, cols(q)],
            send_sem=send_sem.at[k],
            recv_sem=recv_sem.at[k],
            device_id={"tensor": targets[link]},
            device_id_type=MESH,
        )

    def send(name, quarters=None):
        for q in quarters if quarters is not None else ROUTES[name][5]:
            route(name, q).start()

    def arrived(name, quarters=None):
        for q in quarters if quarters is not None else ROUTES[name][5]:
            route(name, q).wait_recv()

    own = [
        pltpu.make_async_copy(tokens_hbm.at[:, cols(q)], xg.at[0, :, cols(q)], load_sem.at[q])
        for q in range(NQ)
    ]
    load_q = pltpu.make_async_copy(wq_hbm, w_in.at[:, pl.ds(0, QC)], load_sem.at[4])
    load_k = pltpu.make_async_copy(wk_hbm, w_in.at[:, pl.ds(QC, HD)], load_sem.at[5])
    load_v = pltpu.make_async_copy(wv_hbm, w_in.at[:, pl.ds(QC + HD, HD)], load_sem.at[6])
    load_kv = pltpu.make_async_copy(kv_hbm, kv, load_sem.at[7])
    load_o = pltpu.make_async_copy(wo_hbm, w_out, load_sem.at[8])
    for copy in (*own, load_q, load_k, load_v, load_kv, load_o):
        copy.start()

    barrier = pltpu.get_barrier_semaphore()
    for link in (UP, DOWN, ACROSS):
        pl.semaphore_signal(barrier, inc=1, device_id={"tensor": targets[link]}, device_id_type=MESH)
    pl.semaphore_wait(barrier, 3)

    for copy in own:
        copy.wait()
    for i in range(NQ):
        for name in ("own_up", "own_down", "own_across"):
            route(name, ROUTES[name][5][i]).start()

    def norm(j):
        def tile(i, c):
            rows = pl.ds(pl.multiple_of(i * 16, 16), 16)
            x = xg[j, rows, :].astype(F32)
            scale = lax.rsqrt(jnp.mean(x * x, axis=-1, keepdims=True) + EPS)
            xn[rows, :] = (x * scale * gain_ref[...].astype(F32)).astype(BF16)
            return c

        lax.fori_loop(0, ROWS_B // 16, tile, 0)

    def rot(m):
        return m * cos_ref[...] + pltpu.roll(m, HD // 2, 1) * sin_ref[...]

    def project():
        def tile(n, c):
            at = pl.ds(pl.multiple_of(n * 256, 256), 256)
            m = jnp.dot(xn[...], w_in[:, at], preferred_element_type=F32)
            turned = jnp.concatenate([rot(m[:, :HD]), rot(m[:, HD:])], 1).astype(BF16)
            qp[:, at] = jnp.dot(pad_ref[...], turned, preferred_element_type=F32).astype(BF16)
            return c

        lax.fori_loop(0, 4, tile, 0)
        m = jnp.dot(xn[...], w_in[:, QC:], preferred_element_type=F32)
        turned = jnp.concatenate([rot(m[:, :HD]), m[:, HD:]], 1).astype(BF16)
        qp[:, QC:] = jnp.dot(pad_ref[...], turned, preferred_element_type=F32).astype(BF16)

    def attend(t):
        inv_root = 1.0 / HD**0.5
        lane = lax.broadcasted_iota(jnp.int32, (HD, 2 * CACHE), 1)
        is_key = lane % 2 == 0
        new_row = lax.broadcasted_iota(jnp.int32, (HD, 16), 0) % 16
        new_lane = lax.broadcasted_iota(jnp.int32, (HD, 16), 1)
        seen = new_lane <= new_row
        contract_last = (((1,), (1,)), ((), ()))

        def seq(s, c):
            rows = pl.ds(pl.multiple_of(s * 16, 16), 16)
            query = jnp.concatenate([qp[rows, h * HD : (h + 1) * HD] for h in range(HEADS)], 0)
            key_new = qp[rows, QC : QC + HD]
            value_new = qp[rows, QC + HD :]
            pairs = kv[t * SEQ_BLOCK + s]
            s_old = lax.dot_general(query, pairs, contract_last, preferred_element_type=F32)
            s_new = lax.dot_general(query, key_new, contract_last, preferred_element_type=F32)
            s_old = jnp.where(is_key, s_old * inv_root, -1e30)
            s_new = jnp.where(seen, s_new * inv_root, -1e30)
            top = jnp.maximum(
                jnp.max(s_old, axis=1, keepdims=True), jnp.max(s_new, axis=1, keepdims=True)
            )
            e_old = jnp.exp(s_old - top)
            e_new = jnp.exp(s_new - top)
            total = jnp.sum(e_old, axis=1, keepdims=True) + jnp.sum(e_new, axis=1, keepdims=True)
            inverse = 1.0 / total
            p_old = pltpu.roll(e_old * inverse, 1, 1).astype(BF16)
            p_new = (e_new * inverse).astype(BF16)
            att = jnp.dot(p_old, pairs, preferred_element_type=F32)
            att = (att + jnp.dot(p_new, value_new, preferred_element_type=F32)).astype(BF16)
            for h in range(HEADS):
                ap[rows, h * HD : (h + 1) * HD] = att[h * 16 : (h + 1) * 16]
            return c

        lax.fori_loop(0, SEQ_BLOCK, seq, 0, unroll=2)
        for n in range(4):
            at = slice(n * 256, (n + 1) * 256)
            ab[:, at] = jnp.dot(
                unpad_ref[...], ap[:, at], preferred_element_type=F32
            ).astype(BF16)

    def powers(t, sign):
        e = exps_ref[pl.ds(pl.multiple_of(t * ROWS_B, ROWS_B), ROWS_B), :]
        if sign < 0:
            return jnp.left_shift(1, -e).astype(F32)
        return jnp.left_shift(1, e + 11).astype(F32) * (2.0**-11)

    def out_project(j, t, after):
        shrink = powers(t, -1)
        for q in (0, 2, 1, 3):
            for half in range(2):
                base = q * CH + half * 512
                part = jnp.dot(
                    ab[...], w_out[:, base : base + 512], preferred_element_type=F32
                )
                for g in range(4):
                    group = base // HD + g
                    scaled = part[:, g * HD : (g + 1) * HD] * shrink[:, group : group + 1]
                    pb[j, :, base + g * HD : base + (g + 1) * HD] = jnp.clip(
                        scaled, -127.0, 127.0
                    ).astype(BF16)
            after(q)

    def add_in(slot, others, q):
        def tile(i, c):
            rows = pl.ds(pl.multiple_of(i * 16, 16), 16)
            total = pb[slot, rows, cols(q)].astype(F32)
            for other in others:
                total = total + rb[other, rows, cols(q)].astype(F32)
            pb[slot, rows, cols(q)] = total.astype(BF16)
            return c

        lax.fori_loop(0, ROWS_B // 16, tile, 0)

    def when(j, k, action):
        pl.when(j == k)(action)

    def before(j):
        @functools.partial(when, j, 1)
        def _():
            arrived("own_up", (0, 1))
            send("far_up")
            arrived("own_down", (2, 3))
            send("far_down")
            arrived("own_up", (2, 3))

        @functools.partial(when, j, 2)
        def _():
            arrived("own_across")
            send("side_up")
            send("side_down")
            arrived("own_down", (0, 1))
            arrived("far_up", (0,))
            send("far_across", (0,))
            arrived("far_down", (2,))
            send("far_across", (2,))

        @functools.partial(when, j, 3)
        def _():
            arrived("far_up", (1,))
            send("far_across", (1,))
            arrived("far_down", (3,))
            send("far_across", (3,))
            send("r_near_down", (2, 3))
            send("r_near_up", (0, 1))

        @functools.partial(when, j, 5)
        def _():
            arrived("far_across")

        @functools.partial(when, j, 6)
        def _():
            arrived("side_up")

        @functools.partial(when, j, 7)
        def _():
            arrived("side_down")
            far_in((0, 2))

    def far_in(quarters):
        for q in quarters:
            arrived("r_far", (q,))
            add_in(4, (R_FAR,), q)
            send("r_half_down" if q < 2 else "r_half_up", (q,))

    def step(j, c):
        dx = (DX_BITS >> j) & 1
        dy = (DY_BITS >> (2 * j)) & 3
        t = ((mx + dx) % 2) * 4 + (my + dy) % 4
        before(j)
        norm(j)
        project()
        attend(t)

        def after(q):
            when(j, 5, lambda: send("r_far", (q,)))
            when(j, 6, lambda: send("r_side_down", (q,)))
            when(j, 7, lambda: send("r_side_up", (q,)))

        out_project(j, t, after)
        return c

    load_q.wait()
    load_k.wait()
    load_v.wait()
    load_kv.wait()
    load_o.wait()
    lax.fori_loop(0, 8, step, 0)

    far_in((1, 3))
    for q in (0, 2, 1, 3):
        arrived("r_side_down", (q,))
        arrived("r_side_up", (q,))
        add_in(3, (R_SIDE_P, R_SIDE_M), q)
        send("r_across", (q,))
        if q < 2:
            arrived("r_half_down", (q,))
            add_in(1, (R_HALF,), q)
            send("r_near_down", (q,))
        else:
            arrived("r_half_up", (q,))
            add_in(2, (R_HALF,), q)
            send("r_near_up", (q,))

    restore = powers(me, 1)
    outs = []
    for q in (0, 2, 1, 3):
        arrived("r_across", (q,))
        arrived("r_near_down", (q,))
        arrived("r_near_up", (q,))
        for g in range(CH // HD):
            group = q * (CH // HD) + g
            at = slice(group * HD, (group + 1) * HD)
            total = pb[0, :, at].astype(F32)
            for r in (R_P, R_M, R_X):
                total = total + rb[r, :, at].astype(F32)
            mixed = xg[0, :, at].astype(F32) + total * restore[:, group : group + 1]
            obuf[:, at] = mixed.astype(BF16)
        copy = pltpu.make_async_copy(obuf.at[:, cols(q)], out_hbm.at[:, cols(q)], out_sem.at[q])
        copy.start()
        outs.append(copy)
    for copy in outs:
        copy.wait()
    for name, spec in ROUTES.items():
        for q in spec[5]:
            route(name, q).wait_send()


def tables():
    position = (np.arange(ROWS_B) % NEW + CACHE).astype(np.float32)
    frequency = THETA ** (-(np.arange(HD // 2, dtype=np.float32) * np.float32(2.0)) / np.float32(HD))
    angles = position[:, None] * frequency.astype(np.float32)[None, :]
    cosine, sine = np.cos(angles), np.sin(angles)
    row = np.arange(ROWS_B)
    padded = row // NEW * 16 + row % NEW
    spread = np.zeros((PADDED, ROWS_B), np.float32)
    spread[padded, row] = 1.0
    return (
        jnp.asarray(np.concatenate([cosine, cosine], 1), F32),
        jnp.asarray(np.concatenate([-sine, sine], 1), F32),
        jnp.asarray(spread, BF16),
        jnp.asarray(spread.T, BF16),
    )


def on_device(
    tokens, norm_gain, query_weight, key_weight, value_weight, out_weight, past_cache, exponents
):
    seqs = past_cache.shape[0]
    pairs = past_cache.reshape(seqs, 2 * CACHE, HD)
    vmem = pl.BlockSpec(memory_space=pltpu.VMEM)
    anywhere = pl.BlockSpec(memory_space=pl.ANY)
    routes = len(ROUTES) * NQ
    return pl.pallas_call(
        body,
        out_shape=jax.ShapeDtypeStruct(tokens.shape, BF16),
        in_specs=[
            anywhere, vmem, anywhere, anywhere, anywhere, anywhere, anywhere, vmem, vmem, vmem,
            vmem, vmem,
        ],
        out_specs=anywhere,
        scratch_shapes=[
            pltpu.VMEM((8, ROWS_B, D), BF16),
            pltpu.VMEM((8, ROWS_B, D), BF16),
            pltpu.VMEM((7, ROWS_B, D), BF16),
            pltpu.VMEM((D, QC + 2 * HD), BF16),
            pltpu.VMEM((QC, D), BF16),
            pltpu.VMEM((seqs, 2 * CACHE, HD), BF16),
            pltpu.VMEM((ROWS_B, D), BF16),
            pltpu.VMEM((PADDED, QC + 2 * HD), BF16),
            pltpu.VMEM((PADDED, QC), BF16),
            pltpu.VMEM((ROWS_B, QC), BF16),
            pltpu.VMEM((ROWS_B, D), BF16),
            pltpu.SemaphoreType.DMA((9,)),
            pltpu.SemaphoreType.DMA((routes,)),
            pltpu.SemaphoreType.DMA((routes,)),
            pltpu.SemaphoreType.DMA((NQ,)),
        ],
        compiler_params=pltpu.CompilerParams(
            collective_id=0, has_side_effects=True, vmem_limit_bytes=67_000_000
        ),
        name="verify_block",
    )(
        tokens, norm_gain.reshape(1, D), query_weight, key_weight, value_weight, out_weight, pairs,
        exponents, *tables(),
    )


def solution(mesh):
    return jax.shard_map(
        on_device,
        mesh=mesh,
        in_specs=(
            P(("dp", "tensor"), None),
            P(),
            P(None, "tensor"),
            P(None, "tensor"),
            P(None, "tensor"),
            P("tensor", None),
            P("dp", None, None, "tensor"),
            P("dp", None),
        ),
        out_specs=P(("dp", "tensor"), None),
        check_vma=False,
    )
```

```python
import functools

import jax
import jax.numpy as jnp
import numpy as np
from jax import lax
from jax.experimental import pallas as pl
from jax.experimental.pallas import tpu as pltpu
from jax.sharding import PartitionSpec as P

HD = 128
NEW = 10
CACHE = 64
D = 4096
HEADS = 8
QC = 1024
SEQ_BLOCK = 16
ROWS_B = 160
PADDED = 256
SPREAD = 512
CH = 1024
NQ = 4
EPS = 1e-05
THETA = 500000.0
MESH = pl.DeviceIdType.MESH
F32 = jnp.float32
BF16 = jnp.bfloat16
SCORE = float(np.log2(np.e) / np.sqrt(HD))

SLOTS = ((0, 0), (0, 3), (0, 1), (1, 0), (0, 2), (1, 2), (1, 3), (1, 1))
DX_BITS = sum(dx << j for j, (dx, _) in enumerate(SLOTS))
DY_BITS = sum(dy << (2 * j) for j, (_, dy) in enumerate(SLOTS))

UP, DOWN, ACROSS, BEYOND, ZUP, ZDOWN, CORE = range(7)
OWN, NEAR_M, NEAR_P, FAR = range(4)
R_HALF, R_P, R_M = range(3)

QUARTERS = [(q * CH, CH) for q in range(NQ)]
SIDE = [(0, 1024), (1024, 1024), (2048, 1024), (3072, 512)]
REST = [(3584, 512)]
ROUTES = {
    "own_up": (UP, "x", 0, "x", 1, QUARTERS),
    "own_down": (DOWN, "x", 0, "x", 2, QUARTERS),
    "own_across": (ACROSS, "x", 0, "x", 3, QUARTERS),
    "far_up": (UP, "x", 1, "x", 4, QUARTERS[:2]),
    "far_down": (DOWN, "x", 2, "x", 4, QUARTERS[2:]),
    "far_across": (ACROSS, "x", 4, "x", 5, QUARTERS),
    "side_up": (UP, "x", 3, "x", 6, SIDE),
    "side_down": (DOWN, "x", 3, "x", 7, SIDE),
    "rest_m": (ACROSS, "x", 1, "x", 6, REST),
    "rest_p": (ACROSS, "x", 2, "x", 7, REST),
    "att_own": (ACROSS, "a", 3, "b", OWN, [(0, QC)]),
    "att_far": (ACROSS, "a", 5, "b", FAR, [(0, QC)]),
    "att_near_m": (ACROSS, "a", 6, "b", NEAR_M, [(0, QC)]),
    "att_near_p": (ACROSS, "a", 7, "b", NEAR_P, [(0, QC)]),
    "half_down": (DOWN, "p", FAR, "r", R_HALF, QUARTERS[:2]),
    "half_up": (UP, "p", FAR, "r", R_HALF, QUARTERS[2:]),
    "sum_down": (DOWN, "p", NEAR_M, "r", R_P, QUARTERS),
    "sum_up": (UP, "p", NEAR_P, "r", R_M, QUARTERS),
}
WEIGHTS = {
    "w_beyond": (BEYOND, True, 0, (0, 1, 2, 3)),
    "w_zup": (ZUP, False, 0, (0, 1, 2, 3)),
    "w_zdown": (ZDOWN, False, 0, (0, 1, 2, 3)),
    "w_fwd_up": (ZUP, False, 3, (0, 1)),
    "w_fwd_down": (ZDOWN, False, 1, (2, 3)),
    "w_core0": (CORE, False, 0, (None,)),
    "w_core3": (CORE, False, 3, (None,)),
    "w_core1": (CORE, False, 1, (None,)),
    "w_core2": (CORE, False, 2, (None,)),
}
BASE = {}
COUNT = 0
for _name, _spec in ROUTES.items():
    BASE[_name] = COUNT
    COUNT += len(_spec[5])
for _name, _spec in WEIGHTS.items():
    BASE[_name] = COUNT
    COUNT += len(_spec[3])
PIECE = QC // 8
SUB = PIECE // 4


def body(
    tokens_hbm, gain_ref, wq_hbm, wk_hbm, wv_hbm, wo_hbm, kv_hbm, exps_ref, cos_ref, sin_ref,
    pad_ref, unpad_ref, pad_k_ref, pad_v_ref, parity_ref, out_hbm,
    xg, pb, rb, ab, bb, w_in, w_out, w_two, kv, xn, qkv, qp, kp, vp, ap, obuf, exps, gains,
    load_sem, send_sem, recv_sem, out_sem,
):
    me = lax.axis_index("tensor")
    mx, my = me // 4, me % 4
    dp = lax.axis_index("dp")
    hi, z, core = dp // 8, (dp // 2) % 4, dp % 2
    other = (1 - mx) * 4 + my
    z_next, z_last = (z + 1) % 4, (z + 3) % 4
    targets = {
        UP: {"tensor": mx * 4 + (my + 1) % 4},
        DOWN: {"tensor": mx * 4 + (my + 3) % 4},
        ACROSS: {"tensor": other},
        BEYOND: {"dp": (1 - hi) * 8 + z * 2 + core, "tensor": other},
        ZUP: {"dp": hi * 8 + z_next * 2 + core},
        ZDOWN: {"dp": hi * 8 + z_last * 2 + core},
        CORE: {"dp": hi * 8 + z * 2 + (1 - core)},
    }
    buffers = {"x": xg, "p": pb, "r": rb, "a": ab, "b": bb}

    def route(name, i):
        k = BASE[name] + i
        if name in ROUTES:
            target, sbuf, sslot, dbuf, dslot, pieces = ROUTES[name]
            at = pl.ds(*pieces[i])
            src, dst = buffers[sbuf].at[sslot, :, at], buffers[dbuf].at[dslot, :, at]
        else:
            target, mine, dz, subs = WEIGHTS[name]
            first = (((z + dz) % 4) * 2 + core) * PIECE
            if subs[i] is None:
                rows = pl.ds(pl.multiple_of(first, PIECE), PIECE)
            else:
                rows = pl.ds(pl.multiple_of(first + subs[i] * SUB, SUB), SUB)
            src, dst = (w_out if mine else w_two).at[rows, :], w_two.at[rows, :]
        return pltpu.make_async_remote_copy(
            src_ref=src, dst_ref=dst, send_sem=send_sem.at[k], recv_sem=recv_sem.at[k],
            device_id=targets[target], device_id_type=MESH,
        )

    def pieces_of(name, which):
        if which is not None:
            return which
        return range(len(ROUTES[name][5] if name in ROUTES else WEIGHTS[name][3]))

    def send(name, which=None):
        for i in pieces_of(name, which):
            route(name, i).start()

    def arrived(name, which=None):
        for i in pieces_of(name, which):
            received(name, i).wait_recv()

    def received(name, i):
        if name in ROUTES:
            return route(name, i)
        k = BASE[name] + i
        target, _, dz, subs = WEIGHTS[name]
        sender_z = {BEYOND: z, ZUP: z_last, ZDOWN: z_next, CORE: z}[target]
        sender_core = (1 - core) if target == CORE else core
        first = (((sender_z + dz) % 4) * 2 + sender_core) * PIECE
        if subs[i] is None:
            rows = pl.ds(pl.multiple_of(first, PIECE), PIECE)
        else:
            rows = pl.ds(pl.multiple_of(first + subs[i] * SUB, SUB), SUB)
        return pltpu.make_async_remote_copy(
            src_ref=w_two.at[rows, :], dst_ref=w_two.at[rows, :], send_sem=send_sem.at[k],
            recv_sem=recv_sem.at[k], device_id=targets[target], device_id_type=MESH,
        )

    load_x = pltpu.make_async_copy(tokens_hbm, xg.at[0], load_sem.at[0])
    load_o = pltpu.make_async_copy(wo_hbm, w_out, load_sem.at[1])
    load_q = pltpu.make_async_copy(wq_hbm, w_in.at[:, pl.ds(0, QC)], load_sem.at[2])
    load_k = pltpu.make_async_copy(wk_hbm, w_in.at[:, pl.ds(QC, HD)], load_sem.at[3])
    load_v = pltpu.make_async_copy(wv_hbm, w_in.at[:, pl.ds(QC + HD, HD)], load_sem.at[4])
    load_kv = pltpu.make_async_copy(kv_hbm, kv, load_sem.at[5])
    for copy in (load_x, load_o, load_q, load_k, load_v, load_kv):
        copy.start()

    barrier = pltpu.get_barrier_semaphore()
    for target in targets.values():
        pl.semaphore_signal(barrier, inc=1, device_id=target, device_id_type=MESH)
    pl.semaphore_wait(barrier, len(targets))

    load_x.wait()
    for i in range(NQ):
        send("own_up", (i,))
        send("own_down", ((i + 2) % NQ,))
        send("own_across", (i,))
    load_o.wait()
    send("w_beyond")

    gain = gain_ref[...].astype(F32)
    for g in range(D // HD):
        gains[:, g * HD : (g + 1) * HD] = jnp.broadcast_to(gain[g : g + 1], (16, HD))
    fill = jnp.zeros((HD - 32, HD), F32)
    for i in range(8 * ROWS_B // HD):
        at = slice(i * HD, (i + 1) * HD)
        exps[at, :] = jnp.concatenate([exps_ref[:, at].astype(F32), fill], 0).T

    def norm(j):
        def some(i5, c):
            scales = []
            for i in range(5):
                rows = pl.ds(pl.multiple_of((i5 * 5 + i) * 16, 16), 16)
                squares = None
                for g in range(D // HD):
                    x = xg[j, rows, g * HD : (g + 1) * HD].astype(F32)
                    squares = x * x if g == 0 else squares + x * x
                scales.append(squares)
            scales = [lax.rsqrt(jnp.sum(s, axis=-1, keepdims=True) * (1.0 / D) + EPS) for s in scales]
            for i in range(5):
                rows = pl.ds(pl.multiple_of((i5 * 5 + i) * 16, 16), 16)
                xn[rows, :] = (xg[j, rows, :].astype(F32) * scales[i] * gains[...]).astype(BF16)
            return c

        lax.fori_loop(0, 2, some, 0)

    def rot(m):
        return m * cos_ref[...] + pltpu.roll(m, HD // 2, 1) * sin_ref[...]

    def project():
        for n in range(5):
            at = slice(n * 256, (n + 1) * 256)
            m = jnp.dot(xn[...], w_in[:, at], preferred_element_type=F32)
            second = rot(m[:, HD:]) if n < 4 else m[:, HD:]
            qkv[:, at] = jnp.concatenate([rot(m[:, :HD]), second], 1).astype(BF16)
        for n in range(4):
            at = slice(n * 256, (n + 1) * 256)
            qp[:, at] = jnp.dot(pad_ref[...], qkv[:, at], preferred_element_type=F32).astype(BF16)
        kp[...] = jnp.dot(
            pad_k_ref[...], qkv[:, QC : QC + HD], preferred_element_type=F32
        ).astype(BF16)
        vp[...] = jnp.dot(pad_v_ref[...], qkv[:, QC + HD :], preferred_element_type=F32).astype(BF16)

    def attend(j, t):
        lane = lax.broadcasted_iota(jnp.int32, (HD, HD), 1)
        token = lax.broadcasted_iota(jnp.int32, (HD, HD), 0) % 16
        seen = (lane % 2 == 0) | (lane <= 2 * token + 1)
        contract_last = (((1,), (1,)), ((), ()))
        batch = 4

        def some(s4, c):
            scores, values = [], []
            for i in range(batch):
                s = s4 * batch + i
                rows = pl.ds(pl.multiple_of(s * 16, 16), 16)
                spread = pl.ds(pl.multiple_of(s * 32, 32), 32)
                query = jnp.concatenate([qp[rows, h * HD : (h + 1) * HD] for h in range(HEADS)], 0)
                pairs = kv[t * SEQ_BLOCK + s]
                keys = jnp.concatenate([pairs[:32] * parity_ref[0] + kp[spread, :], pairs[32:]], 0)
                values.append(
                    jnp.concatenate([pairs[:32] * parity_ref[1] + vp[spread, :], pairs[32:]], 0)
                )
                scores.append(
                    lax.dot_general(query, keys, contract_last, preferred_element_type=F32)
                )
            scores = [jnp.where(seen, x, -1e30) for x in scores]
            tops = [jnp.max(x, axis=1, keepdims=True) for x in scores]
            raised = [jnp.exp2((x - top) * SCORE) for x, top in zip(scores, tops)]
            totals = [jnp.sum(x, axis=1, keepdims=True) for x in raised]
            probs = [(x * (1.0 / total)).astype(BF16) for x, total in zip(raised, totals)]
            for i in range(batch):
                rows = pl.ds(pl.multiple_of((s4 * batch + i) * 16, 16), 16)
                p = pltpu.roll(probs[i], 1, 1)
                att = jnp.dot(p, values[i], preferred_element_type=F32).astype(BF16)
                for h in range(HEADS):
                    ap[rows, h * HD : (h + 1) * HD] = att[h * 16 : (h + 1) * 16]
            return c

        lax.fori_loop(0, SEQ_BLOCK // batch, some, 0)
        for n in range(4):
            at = slice(n * 256, (n + 1) * 256)
            ab[j, :, at] = jnp.dot(
                unpad_ref[...], ap[:, at], preferred_element_type=F32
            ).astype(BF16)

    def powers(t, sign):
        e = exps[pl.ds(pl.multiple_of(t * ROWS_B, ROWS_B), ROWS_B), :].astype(jnp.int32)
        if sign < 0:
            return jnp.left_shift(1, -e).astype(F32)
        return jnp.left_shift(1, e + 11).astype(F32) * (2.0**-11)

    def out_project(att, weights, k, t, order, extra, done):
        shrink = powers(t, -1)
        for q in order:
            for base in (q * CH, q * CH + 512):
                part = jnp.dot(att, weights[:, base : base + 512], preferred_element_type=F32)
                for g in range(4):
                    at = slice(base + g * HD, base + (g + 1) * HD)
                    group = base // HD + g
                    scaled = part[:, g * HD : (g + 1) * HD] * shrink[:, group : group + 1]
                    scaled = jnp.clip(scaled, -127.0, 127.0).astype(BF16)
                    for r in extra(q, g == 0 and base == q * CH):
                        scaled = scaled.astype(F32) + r[:, at].astype(F32)
                    pb[k, :, at] = scaled.astype(BF16)
            done(q)

    def column_block(j):
        return j - (j // 4)

    def second(k, dy, order, half, name):
        t = mx * 4 + (my + dy) % 4

        def extra(q, first):
            refs = [pb.at[k]]
            if half is not None and q in half[1]:
                if first:
                    arrived(half[0], (half[1].index(q),))
                refs.append(rb.at[R_HALF])
            return refs

        def done(q):
            if name == "half":
                send("half_down" if q < 2 else "half_up", (q % 2,))
            elif name:
                send(name, (q,))

        out_project(bb[k], w_two, k, t, order, extra, done)

    def when(j, k, action):
        pl.when(j == k)(action)

    def before(j):
        @functools.partial(when, j, 1)
        def _():
            arrived("own_up", (0,))
            send("far_up", (0,))
            arrived("own_down", (2,))
            send("far_down", (0,))
            for i in range(4):
                arrived("w_beyond", (i,))
                send("w_zup", (i,))
                send("w_zdown", (i,))
                if i == 1:
                    arrived("own_up", (1,))
                    send("far_up", (1,))
                    arrived("own_down", (3,))
                    send("far_down", (1,))
            send("w_core0")
            arrived("own_up", (2, 3))
            send("rest_m")
            arrived("own_down", (0, 1))
            send("rest_p")
            arrived("own_across")
            send("side_up")
            send("side_down")

        @functools.partial(when, j, 2)
        def _():
            arrived("far_up", (0,))
            send("far_across", (0,))
            arrived("far_down", (0,))
            send("far_across", (2,))
            arrived("w_zup", (0, 1))
            send("w_fwd_up")
            arrived("w_zdown", (2, 3))
            send("w_fwd_down")

        @functools.partial(when, j, 3)
        def _():
            arrived("far_up", (1,))
            send("far_across", (1,))
            arrived("far_down", (1,))
            send("far_across", (3,))

        @functools.partial(when, j, 4)
        def _():
            send("att_own")
            arrived("w_zup", (2, 3))
            send("w_core3")
            arrived("w_zdown", (0, 1))
            send("w_core1")

        @functools.partial(when, j, 5)
        def _():
            arrived("w_fwd_up")
            arrived("w_fwd_down")
            send("w_core2")
            arrived("far_across")

        @functools.partial(when, j, 6)
        def _():
            send("att_far")
            arrived("rest_m")
            arrived("side_up")

        @functools.partial(when, j, 7)
        def _():
            send("att_near_m")
            for name in ("w_core0", "w_core3", "w_core1", "w_core2"):
                arrived(name)
            arrived("att_far")
            second(FAR, 2, (0, 2, 1, 3), None, "half")
            arrived("rest_p")
            arrived("side_down")

    def step(j, c):
        dx = (DX_BITS >> j) & 1
        dy = (DY_BITS >> (2 * j)) & 3
        t = ((mx + dx) % 2) * 4 + (my + dy) % 4
        before(j)
        norm(j)
        project()
        attend(j, t)

        @pl.when(dx == 0)
        def _():
            out_project(
                ab[j], w_out, column_block(j), t, range(NQ), lambda q, first: (), lambda q: None
            )

        return c

    load_q.wait()
    load_k.wait()
    load_v.wait()
    load_kv.wait()
    lax.fori_loop(0, 8, step, 0)

    send("att_near_p")
    arrived("att_near_m")
    second(NEAR_M, 3, (2, 3, 0, 1), ("half_down", (0, 1)), "sum_down")
    arrived("att_own")
    second(OWN, 0, range(NQ), None, None)
    arrived("att_near_p")
    second(NEAR_P, 1, (0, 1, 2, 3), ("half_up", (2, 3)), "sum_up")

    restore = powers(me, 1)
    outs = []
    for q in range(NQ):
        arrived("sum_down", (q,))
        arrived("sum_up", (q,))
        for g in range(CH // HD):
            group = q * (CH // HD) + g
            at = slice(group * HD, (group + 1) * HD)
            total = pb[OWN, :, at].astype(F32)
            for r in (R_P, R_M):
                total = total + rb[r, :, at].astype(F32)
            mixed = xg[0, :, at].astype(F32) + total * restore[:, group : group + 1]
            obuf[:, at] = mixed.astype(BF16)
        at = pl.ds(*QUARTERS[q])
        copy = pltpu.make_async_copy(obuf.at[:, at], out_hbm.at[:, at], out_sem.at[q])
        copy.start()
        outs.append(copy)
    for copy in outs:
        copy.wait()
    for name in (*ROUTES, *WEIGHTS):
        for i in pieces_of(name, None):
            route(name, i).wait_send()


def tables():
    position = (np.arange(ROWS_B) % NEW + CACHE).astype(np.float32)
    frequency = THETA ** (-(np.arange(HD // 2, dtype=np.float32) * np.float32(2.0)) / np.float32(HD))
    angles = position[:, None] * frequency.astype(np.float32)[None, :]
    cosine, sine = np.cos(angles), np.sin(angles)
    row = np.arange(ROWS_B)
    spread = np.zeros((PADDED, ROWS_B), np.float32)
    spread[row // NEW * 16 + row % NEW, row] = 1.0
    keys = np.zeros((SPREAD, ROWS_B), np.float32)
    keys[row // NEW * 32 + 2 * (row % NEW) + 1, row] = 1.0
    values = np.zeros((SPREAD, ROWS_B), np.float32)
    values[row // NEW * 32 + 2 * (row % NEW) + 2, row] = 1.0
    even = np.broadcast_to((np.arange(32) % 2 == 0)[:, None], (32, HD))
    return (
        jnp.asarray(np.concatenate([cosine, cosine], 1), F32),
        jnp.asarray(np.concatenate([-sine, sine], 1), F32),
        jnp.asarray(spread, BF16),
        jnp.asarray(spread.T, BF16),
        jnp.asarray(keys, BF16),
        jnp.asarray(values, BF16),
        jnp.asarray(np.stack([even, ~even]), BF16),
    )


def on_device(
    tokens, norm_gain, query_weight, key_weight, value_weight, out_weight, past_cache, exponents
):
    seqs = past_cache.shape[0]
    pairs = past_cache.reshape(seqs, 2 * CACHE, HD)
    vmem = pl.BlockSpec(memory_space=pltpu.VMEM)
    anywhere = pl.BlockSpec(memory_space=pl.ANY)
    return pl.pallas_call(
        body,
        out_shape=jax.ShapeDtypeStruct(tokens.shape, BF16),
        in_specs=[anywhere, vmem, *[anywhere] * 5, *[vmem] * 8],
        out_specs=anywhere,
        scratch_shapes=[
            pltpu.VMEM((8, ROWS_B, D), BF16),
            pltpu.VMEM((4, ROWS_B, D), BF16),
            pltpu.VMEM((3, ROWS_B, D), BF16),
            pltpu.VMEM((8, ROWS_B, QC), BF16),
            pltpu.VMEM((4, ROWS_B, QC), BF16),
            pltpu.VMEM((D, QC + 2 * HD), BF16),
            pltpu.VMEM((QC, D), BF16),
            pltpu.VMEM((QC, D), BF16),
            pltpu.VMEM((seqs, 2 * CACHE, HD), BF16),
            pltpu.VMEM((ROWS_B, D), BF16),
            pltpu.VMEM((ROWS_B, QC + 2 * HD), BF16),
            pltpu.VMEM((PADDED, QC), BF16),
            pltpu.VMEM((SPREAD, HD), BF16),
            pltpu.VMEM((SPREAD, HD), BF16),
            pltpu.VMEM((PADDED, QC), BF16),
            pltpu.VMEM((ROWS_B, D), BF16),
            pltpu.VMEM((8 * ROWS_B, HD), F32),
            pltpu.VMEM((16, D), F32),
            pltpu.SemaphoreType.DMA((6,)),
            pltpu.SemaphoreType.DMA((COUNT,)),
            pltpu.SemaphoreType.DMA((COUNT,)),
            pltpu.SemaphoreType.DMA((NQ,)),
        ],
        compiler_params=pltpu.CompilerParams(
            collective_id=0, has_side_effects=True, vmem_limit_bytes=67_000_000
        ),
        name="verify_block",
    )(
        tokens, norm_gain.reshape(D // HD, HD), query_weight, key_weight, value_weight, out_weight,
        pairs, exponents.T, *tables(),
    )


def solution(mesh):
    return jax.shard_map(
        on_device,
        mesh=mesh,
        in_specs=(
            P(("dp", "tensor"), None),
            P(),
            P(None, "tensor"),
            P(None, "tensor"),
            P(None, "tensor"),
            P("tensor", None),
            P("dp", None, None, "tensor"),
            P("dp", None),
        ),
        out_specs=P(("dp", "tensor"), None),
        check_vma=False,
    )
```

```python
import functools

import jax
import jax.numpy as jnp
import numpy as np
from jax import lax
from jax.experimental import pallas as pl
from jax.experimental.pallas import tpu as pltpu
from jax.sharding import PartitionSpec as P

HD = 128
NEW = 10
CACHE = 64
D = 4096
HEADS = 8
QC = 1024
SEQ_BLOCK = 16
ROWS_B = 160
PADDED = 256
SPREAD = 512
CH = 1024
NQ = 4
EPS = 1e-05
THETA = 500000.0
MESH = pl.DeviceIdType.MESH
F32 = jnp.float32
BF16 = jnp.bfloat16
SCORE = float(np.log2(np.e) / np.sqrt(HD))

SLOTS = ((0, 0), (1, 0), (0, 2), (0, 3), (0, 1), (1, 2), (1, 3), (1, 1))
DX_BITS = sum(dx << j for j, (dx, _) in enumerate(SLOTS))
DY_BITS = sum(dy << (2 * j) for j, (_, dy) in enumerate(SLOTS))

UP, DOWN, ACROSS, BEYOND, ZUP, ZDOWN, CORE = range(7)
OWN, FAR, NEAR_M, NEAR_P = range(4)
R_HALF, R_P, R_M = range(3)

QUARTERS = [(q * CH, CH) for q in range(NQ)]
SIDE = [(0, 1024), (1024, 1024), (2048, 1024), (3072, 512)]
REST = [(3584, 512)]
HALVES = [(0, 80), (80, 80)]
ROUTES = {
    "own_up": (UP, "x", 0, "x", 3, QUARTERS),
    "own_down": (DOWN, "x", 0, "x", 4, QUARTERS),
    "own_across": (ACROSS, "x", 0, "x", 1, QUARTERS),
    "far_up": (UP, "x", 3, "x", 2, QUARTERS[:2]),
    "far_down": (DOWN, "x", 4, "x", 2, QUARTERS[2:]),
    "far_across": (ACROSS, "x", 2, "x", 5, QUARTERS),
    "side_up": (UP, "x", 1, "x", 6, SIDE),
    "side_down": (DOWN, "x", 1, "x", 7, SIDE),
    "rest_m": (ACROSS, "x", 3, "x", 6, REST),
    "rest_p": (ACROSS, "x", 4, "x", 7, REST),
    "att_own": (ACROSS, "a", 1, "b", OWN, HALVES),
    "att_far": (ACROSS, "a", 5, "b", FAR, HALVES),
    "att_near_m": (ACROSS, "a", 6, "b", NEAR_M, HALVES),
    "att_near_p": (ACROSS, "a", 7, "b", NEAR_P, HALVES),
    "half_down": (DOWN, "p", FAR, "r", R_HALF, QUARTERS[:2]),
    "half_up": (UP, "p", FAR, "r", R_HALF, QUARTERS[2:]),
    "sum_down": (DOWN, "p", NEAR_M, "r", R_P, QUARTERS),
    "sum_up": (UP, "p", NEAR_P, "r", R_M, QUARTERS),
}
WEIGHTS = {
    "w_beyond": (BEYOND, True, 0, (0, 1, 2, 3)),
    "w_zup": (ZUP, False, 0, (0, 1, 2, 3)),
    "w_zdown": (ZDOWN, False, 0, (0, 1, 2, 3)),
    "w_fwd_up": (ZUP, False, 3, (0, 1)),
    "w_fwd_down": (ZDOWN, False, 1, (2, 3)),
    "w_core0": (CORE, False, 0, (None,)),
    "w_core3": (CORE, False, 3, (None,)),
    "w_core1": (CORE, False, 1, (None,)),
    "w_core2": (CORE, False, 2, (None,)),
}
BASE = {}
COUNT = 0
for _name, _spec in ROUTES.items():
    BASE[_name] = COUNT
    COUNT += len(_spec[5])
for _name, _spec in WEIGHTS.items():
    BASE[_name] = COUNT
    COUNT += len(_spec[3])
PIECE = QC // 8
SUB = PIECE // 4


def body(
    tokens_hbm, gain_ref, wq_hbm, wk_hbm, wv_hbm, wo_hbm, kv_hbm, exps_ref, cos_ref, sin_ref,
    pad_ref, unpad_ref, pad_k_ref, pad_v_ref, parity_ref, out_hbm,
    xg, pb, rb, ab, bb, w_in, w_out, w_two, kv, xn, qkv, qp, kp, vp, ap, exps, gains,
    load_sem, send_sem, recv_sem, out_sem,
):
    obuf = xn
    me = lax.axis_index("tensor")
    mx, my = me // 4, me % 4
    dp = lax.axis_index("dp")
    hi, z, core = dp // 8, (dp // 2) % 4, dp % 2
    other = (1 - mx) * 4 + my
    z_next, z_last = (z + 1) % 4, (z + 3) % 4
    targets = {
        UP: {"tensor": mx * 4 + (my + 1) % 4},
        DOWN: {"tensor": mx * 4 + (my + 3) % 4},
        ACROSS: {"tensor": other},
        BEYOND: {"dp": (1 - hi) * 8 + z * 2 + core, "tensor": other},
        ZUP: {"dp": hi * 8 + z_next * 2 + core},
        ZDOWN: {"dp": hi * 8 + z_last * 2 + core},
        CORE: {"dp": hi * 8 + z * 2 + (1 - core)},
    }
    buffers = {"x": xg, "p": pb, "r": rb, "a": ab, "b": bb}

    def route(name, i):
        k = BASE[name] + i
        if name in ROUTES:
            target, sbuf, sslot, dbuf, dslot, pieces = ROUTES[name]
            at = pl.ds(*pieces[i])
            if sbuf == "a":
                src, dst = ab.at[sslot, at, :], bb.at[dslot, at, :]
            else:
                src, dst = buffers[sbuf].at[sslot, :, at], buffers[dbuf].at[dslot, :, at]
        else:
            target, mine, dz, subs = WEIGHTS[name]
            first = (((z + dz) % 4) * 2 + core) * PIECE
            if subs[i] is None:
                rows = pl.ds(pl.multiple_of(first, PIECE), PIECE)
            else:
                rows = pl.ds(pl.multiple_of(first + subs[i] * SUB, SUB), SUB)
            src, dst = (w_out if mine else w_two).at[rows, :], w_two.at[rows, :]
        return pltpu.make_async_remote_copy(
            src_ref=src, dst_ref=dst, send_sem=send_sem.at[k], recv_sem=recv_sem.at[k],
            device_id=targets[target], device_id_type=MESH,
        )

    def pieces_of(name, which):
        if which is not None:
            return which
        return range(len(ROUTES[name][5] if name in ROUTES else WEIGHTS[name][3]))

    def send(name, which=None):
        for i in pieces_of(name, which):
            route(name, i).start()

    def arrived(name, which=None):
        for i in pieces_of(name, which):
            received(name, i).wait_recv()

    def received(name, i):
        if name in ROUTES:
            return route(name, i)
        k = BASE[name] + i
        target, _, dz, subs = WEIGHTS[name]
        sender_z = {BEYOND: z, ZUP: z_last, ZDOWN: z_next, CORE: z}[target]
        sender_core = (1 - core) if target == CORE else core
        first = (((sender_z + dz) % 4) * 2 + sender_core) * PIECE
        if subs[i] is None:
            rows = pl.ds(pl.multiple_of(first, PIECE), PIECE)
        else:
            rows = pl.ds(pl.multiple_of(first + subs[i] * SUB, SUB), SUB)
        return pltpu.make_async_remote_copy(
            src_ref=w_two.at[rows, :], dst_ref=w_two.at[rows, :], send_sem=send_sem.at[k],
            recv_sem=recv_sem.at[k], device_id=targets[target], device_id_type=MESH,
        )

    load_x = pltpu.make_async_copy(tokens_hbm, xg.at[0], load_sem.at[0])
    load_o = pltpu.make_async_copy(wo_hbm, w_out, load_sem.at[1])
    load_q = pltpu.make_async_copy(wq_hbm, w_in.at[:, pl.ds(0, QC)], load_sem.at[2])
    load_k = pltpu.make_async_copy(wk_hbm, w_in.at[:, pl.ds(QC, HD)], load_sem.at[3])
    load_v = pltpu.make_async_copy(wv_hbm, w_in.at[:, pl.ds(QC + HD, HD)], load_sem.at[4])
    load_kv = pltpu.make_async_copy(kv_hbm, kv, load_sem.at[5])
    for copy in (load_x, load_o, load_q, load_k, load_v, load_kv):
        copy.start()

    barrier = pltpu.get_barrier_semaphore()
    for target in targets.values():
        pl.semaphore_signal(barrier, inc=1, device_id=target, device_id_type=MESH)
    pl.semaphore_wait(barrier, len(targets))

    load_x.wait()
    for i in range(NQ):
        if i < 2:
            send("own_up", (i,))
            send("own_down", (i + 2,))
        send("own_across", (i,))
    load_o.wait()
    send("w_beyond")

    gain = gain_ref[...].astype(F32)
    for g in range(D // HD):
        gains[:, g * HD : (g + 1) * HD] = jnp.broadcast_to(gain[g : g + 1], (16, HD))
    fill = jnp.zeros((HD - 32, HD), F32)
    for i in range(8 * ROWS_B // HD):
        at = slice(i * HD, (i + 1) * HD)
        exps[at, :] = jnp.concatenate([exps_ref[:, at].astype(F32), fill], 0).T

    def norm(j):
        def some(i5, c):
            scales = []
            for i in range(5):
                rows = pl.ds(pl.multiple_of((i5 * 5 + i) * 16, 16), 16)
                squares = None
                for g in range(D // HD):
                    x = xg[j, rows, g * HD : (g + 1) * HD].astype(F32)
                    squares = x * x if g == 0 else squares + x * x
                scales.append(squares)
            scales = [lax.rsqrt(jnp.sum(s, axis=-1, keepdims=True) * (1.0 / D) + EPS) for s in scales]
            for i in range(5):
                rows = pl.ds(pl.multiple_of((i5 * 5 + i) * 16, 16), 16)
                xn[rows, :] = (xg[j, rows, :].astype(F32) * scales[i] * gains[...]).astype(BF16)
            return c

        lax.fori_loop(0, 2, some, 0)

    def rot(m):
        return m * cos_ref[...] + pltpu.roll(m, HD // 2, 1) * sin_ref[...]

    def project():
        for n in range(5):
            at = slice(n * 256, (n + 1) * 256)
            m = jnp.dot(xn[...], w_in[:, at], preferred_element_type=F32)
            second = rot(m[:, HD:]) if n < 4 else m[:, HD:]
            qkv[:, at] = jnp.concatenate([rot(m[:, :HD]), second], 1).astype(BF16)
        for n in range(4):
            at = slice(n * 256, (n + 1) * 256)
            qp[:, at] = jnp.dot(pad_ref[...], qkv[:, at], preferred_element_type=F32).astype(BF16)
        kp[...] = jnp.dot(
            pad_k_ref[...], qkv[:, QC : QC + HD], preferred_element_type=F32
        ).astype(BF16)
        vp[...] = jnp.dot(pad_v_ref[...], qkv[:, QC + HD :], preferred_element_type=F32).astype(BF16)

    def attend(j, t, half):
        lane = lax.broadcasted_iota(jnp.int32, (HD, HD), 1)
        token = lax.broadcasted_iota(jnp.int32, (HD, HD), 0) % 16
        seen = (lane % 2 == 0) | (lane <= 2 * token + 1)
        contract_last = (((1,), (1,)), ((), ()))
        batch = 4

        def some(s4, c):
            scores, values = [], []
            for i in range(batch):
                s = s4 * batch + i
                rows = pl.ds(pl.multiple_of(s * 16, 16), 16)
                spread = pl.ds(pl.multiple_of(s * 32, 32), 32)
                query = jnp.concatenate([qp[rows, h * HD : (h + 1) * HD] for h in range(HEADS)], 0)
                pairs = kv[t * SEQ_BLOCK + s]
                keys = jnp.concatenate([pairs[:32] * parity_ref[0] + kp[spread, :], pairs[32:]], 0)
                values.append(
                    jnp.concatenate([pairs[:32] * parity_ref[1] + vp[spread, :], pairs[32:]], 0)
                )
                scores.append(
                    lax.dot_general(query, keys, contract_last, preferred_element_type=F32)
                )
            scores = [jnp.where(seen, x, -1e30) for x in scores]
            tops = [jnp.max(x, axis=1, keepdims=True) for x in scores]
            raised = [jnp.exp2((x - top) * SCORE) for x, top in zip(scores, tops)]
            totals = [jnp.sum(x, axis=1, keepdims=True) for x in raised]
            probs = [(x * (1.0 / total)).astype(BF16) for x, total in zip(raised, totals)]
            for i in range(batch):
                rows = pl.ds(pl.multiple_of((s4 * batch + i) * 16, 16), 16)
                p = pltpu.roll(probs[i], 1, 1)
                att = jnp.dot(p, values[i], preferred_element_type=F32).astype(BF16)
                for h in range(HEADS):
                    ap[rows, h * HD : (h + 1) * HD] = att[h * 16 : (h + 1) * 16]
            return c

        parts = SEQ_BLOCK // batch // 2
        lax.fori_loop(half * parts, (half + 1) * parts, some, 0)
        rows = slice(half * 80, (half + 1) * 80)
        for n in range(4):
            at = slice(n * 256, (n + 1) * 256)
            padded = ap[half * 128 : (half + 1) * 128, at]
            ab[j, rows, at] = jnp.dot(
                unpad_ref[...], padded, preferred_element_type=F32
            ).astype(BF16)

    def powers(t, sign):
        e = exps[pl.ds(pl.multiple_of(t * ROWS_B, ROWS_B), ROWS_B), :].astype(jnp.int32)
        if sign < 0:
            return jnp.left_shift(1, -e).astype(F32)
        return jnp.left_shift(1, e + 11).astype(F32) * (2.0**-11)

    def out_project(att, weights, k, t, order, extra, done):
        shrink = powers(t, -1)
        for q in order:
            for base in (q * CH, q * CH + 512):
                part = jnp.dot(att, weights[:, base : base + 512], preferred_element_type=F32)
                for g in range(4):
                    at = slice(base + g * HD, base + (g + 1) * HD)
                    group = base // HD + g
                    scaled = part[:, g * HD : (g + 1) * HD] * shrink[:, group : group + 1]
                    scaled = jnp.clip(scaled, -127.0, 127.0).astype(BF16)
                    for r in extra(q, g == 0 and base == q * CH):
                        scaled = scaled.astype(F32) + r[:, at].astype(F32)
                    pb[k, :, at] = scaled.astype(BF16)
            done(q)

    def column_block(j):
        return j - (j + 7) // 8

    def second(k, dy, order, half, name):
        t = mx * 4 + (my + dy) % 4

        def extra(q, first):
            refs = [pb.at[k]]
            if half is not None and q in half[1]:
                if first:
                    arrived(half[0], (half[1].index(q),))
                refs.append(rb.at[R_HALF])
            return refs

        def done(q):
            if name == "half":
                send("half_down" if q < 2 else "half_up", (q % 2,))
            elif name:
                send(name, (q,))

        out_project(bb[k], w_two, k, t, order, extra, done)

    def when(j, k, action):
        pl.when(j == k)(action)

    def before(j):
        @functools.partial(when, j, 1)
        def _():
            arrived("own_up", (0,))
            send("far_up", (0,))
            send("own_up", (2,))
            arrived("own_down", (2,))
            send("far_down", (0,))
            send("own_down", (0,))
            for i in range(4):
                arrived("w_beyond", (i,))
                send("w_zup", (i,))
                send("w_zdown", (i,))
                if i == 1:
                    arrived("own_up", (1,))
                    send("far_up", (1,))
                    send("own_up", (3,))
                    arrived("own_down", (3,))
                    send("far_down", (1,))
                    send("own_down", (1,))
            send("w_core0")
            arrived("far_up", (0,))
            send("far_across", (0,))
            arrived("far_down", (0,))
            send("far_across", (2,))
            arrived("own_across")
            send("side_up")
            send("side_down")

        @functools.partial(when, j, 2)
        def _():
            arrived("far_up", (1,))
            send("far_across", (1,))
            arrived("far_down", (1,))
            send("far_across", (3,))
            arrived("w_zup", (0, 1))
            send("w_fwd_up")
            arrived("w_zdown", (2, 3))
            send("w_fwd_down")

        @functools.partial(when, j, 3)
        def _():
            arrived("own_up", (2, 3))
            send("rest_m")
            arrived("own_down", (0, 1))
            send("rest_p")
            arrived("w_zup", (2, 3))
            send("w_core3")
            arrived("w_zdown", (0, 1))
            send("w_core1")

        @functools.partial(when, j, 5)
        def _():
            arrived("w_fwd_up")
            arrived("w_fwd_down")
            send("w_core2")
            arrived("far_across")

        @functools.partial(when, j, 6)
        def _():
            arrived("rest_m")
            arrived("side_up")

        @functools.partial(when, j, 7)
        def _():
            for name in ("w_core0", "w_core3", "w_core1", "w_core2"):
                arrived(name)
            arrived("att_far")
            second(FAR, 2, (0, 2, 1, 3), None, "half")
            arrived("rest_p")
            arrived("side_down")

    def step(j, c):
        dx = (DX_BITS >> j) & 1
        dy = (DY_BITS >> (2 * j)) & 3
        t = ((mx + dx) % 2) * 4 + (my + dy) % 4
        before(j)
        norm(j)
        project()
        for half in range(2):
            attend(j, t, half)
            for slot, name in ((5, "att_far"), (6, "att_near_m"), (7, "att_near_p")):
                when(j, slot, functools.partial(send, name, (half,)))

        @pl.when(dx == 0)
        def _():
            out_project(
                ab[j], w_out, column_block(j), t, range(NQ), lambda q, first: (), lambda q: None
            )

        return c

    load_q.wait()
    load_k.wait()
    load_v.wait()
    load_kv.wait()
    lax.fori_loop(0, 8, step, 0)

    send("att_own")
    arrived("att_near_m")
    second(NEAR_M, 3, (2, 3, 0, 1), ("half_down", (0, 1)), "sum_down")
    arrived("att_near_p")
    second(NEAR_P, 1, (0, 1, 2, 3), ("half_up", (2, 3)), "sum_up")
    arrived("att_own")
    second(OWN, 0, range(NQ), None, None)

    restore = powers(me, 1)
    outs = []
    for q in range(NQ):
        arrived("sum_down", (q,))
        arrived("sum_up", (q,))
        for g in range(CH // HD):
            group = q * (CH // HD) + g
            at = slice(group * HD, (group + 1) * HD)
            total = pb[OWN, :, at].astype(F32)
            for r in (R_P, R_M):
                total = total + rb[r, :, at].astype(F32)
            mixed = xg[0, :, at].astype(F32) + total * restore[:, group : group + 1]
            obuf[:, at] = mixed.astype(BF16)
        at = pl.ds(*QUARTERS[q])
        copy = pltpu.make_async_copy(obuf.at[:, at], out_hbm.at[:, at], out_sem.at[q])
        copy.start()
        outs.append(copy)
    for copy in outs:
        copy.wait()
    for name in (*ROUTES, *WEIGHTS):
        for i in pieces_of(name, None):
            route(name, i).wait_send()


def tables():
    position = (np.arange(ROWS_B) % NEW + CACHE).astype(np.float32)
    frequency = THETA ** (-(np.arange(HD // 2, dtype=np.float32) * np.float32(2.0)) / np.float32(HD))
    angles = position[:, None] * frequency.astype(np.float32)[None, :]
    cosine, sine = np.cos(angles), np.sin(angles)
    row = np.arange(ROWS_B)
    spread = np.zeros((PADDED, ROWS_B), np.float32)
    spread[row // NEW * 16 + row % NEW, row] = 1.0
    keys = np.zeros((SPREAD, ROWS_B), np.float32)
    keys[row // NEW * 32 + 2 * (row % NEW) + 1, row] = 1.0
    values = np.zeros((SPREAD, ROWS_B), np.float32)
    values[row // NEW * 32 + 2 * (row % NEW) + 2, row] = 1.0
    even = np.broadcast_to((np.arange(32) % 2 == 0)[:, None], (32, HD))
    return (
        jnp.asarray(np.concatenate([cosine, cosine], 1), F32),
        jnp.asarray(np.concatenate([-sine, sine], 1), F32),
        jnp.asarray(spread, BF16),
        jnp.asarray(spread.T[: ROWS_B // 2, : PADDED // 2], BF16),
        jnp.asarray(keys, BF16),
        jnp.asarray(values, BF16),
        jnp.asarray(np.stack([even, ~even]), BF16),
    )


def on_device(
    tokens, norm_gain, query_weight, key_weight, value_weight, out_weight, past_cache, exponents
):
    seqs = past_cache.shape[0]
    pairs = past_cache.reshape(seqs, 2 * CACHE, HD)
    vmem = pl.BlockSpec(memory_space=pltpu.VMEM)
    anywhere = pl.BlockSpec(memory_space=pl.ANY)
    return pl.pallas_call(
        body,
        out_shape=jax.ShapeDtypeStruct(tokens.shape, BF16),
        in_specs=[anywhere, vmem, *[anywhere] * 5, *[vmem] * 8],
        out_specs=anywhere,
        scratch_shapes=[
            pltpu.VMEM((8, ROWS_B, D), BF16),
            pltpu.VMEM((4, ROWS_B, D), BF16),
            pltpu.VMEM((3, ROWS_B, D), BF16),
            pltpu.VMEM((8, ROWS_B, QC), BF16),
            pltpu.VMEM((4, ROWS_B, QC), BF16),
            pltpu.VMEM((D, QC + 2 * HD), BF16),
            pltpu.VMEM((QC, D), BF16),
            pltpu.VMEM((QC, D), BF16),
            pltpu.VMEM((seqs, 2 * CACHE, HD), BF16),
            pltpu.VMEM((ROWS_B, D), BF16),
            pltpu.VMEM((ROWS_B, QC + 2 * HD), BF16),
            pltpu.VMEM((PADDED, QC), BF16),
            pltpu.VMEM((SPREAD, HD), BF16),
            pltpu.VMEM((SPREAD, HD), BF16),
            pltpu.VMEM((PADDED, QC), BF16),
            pltpu.VMEM((8 * ROWS_B, HD), F32),
            pltpu.VMEM((16, D), F32),
            pltpu.SemaphoreType.DMA((6,)),
            pltpu.SemaphoreType.DMA((COUNT,)),
            pltpu.SemaphoreType.DMA((COUNT,)),
            pltpu.SemaphoreType.DMA((NQ,)),
        ],
        compiler_params=pltpu.CompilerParams(
            collective_id=0, has_side_effects=True, vmem_limit_bytes=67_000_000
        ),
        name="verify_block",
    )(
        tokens, norm_gain.reshape(D // HD, HD), query_weight, key_weight, value_weight, out_weight,
        pairs, exponents.T, *tables(),
    )


def solution(mesh):
    return jax.shard_map(
        on_device,
        mesh=mesh,
        in_specs=(
            P(("dp", "tensor"), None),
            P(),
            P(None, "tensor"),
            P(None, "tensor"),
            P(None, "tensor"),
            P("tensor", None),
            P("dp", None, None, "tensor"),
            P("dp", None),
        ),
        out_specs=P(("dp", "tensor"), None),
        check_vma=False,
    )
```

```python
import functools

import jax
import jax.numpy as jnp
import numpy as np
from jax import lax
from jax.experimental import pallas as pl
from jax.experimental.pallas import tpu as pltpu
from jax.sharding import PartitionSpec as P

HD = 128
NEW = 10
CACHE = 64
D = 4096
HEADS = 8
QC = 1024
SEQ_BLOCK = 16
ROWS_B = 160
PADDED = 256
SPREAD = 512
CH = 1024
NQ = 4
EPS = 1e-05
THETA = 500000.0
MESH = pl.DeviceIdType.MESH
F32 = jnp.float32
BF16 = jnp.bfloat16
SCORE = float(np.log2(np.e) / np.sqrt(HD))

SLOTS = ((0, 0), (0, 2), (0, 3), (1, 2), (0, 1), (1, 3), (1, 1), (1, 0))
DX_BITS = sum(dx << j for j, (dx, _) in enumerate(SLOTS))
DY_BITS = sum(dy << (2 * j) for j, (_, dy) in enumerate(SLOTS))

UP, DOWN, ACROSS, BEYOND, ZUP, ZDOWN, CORE = range(7)
OWN, FAR, NEAR_M, NEAR_P = range(4)
R_HALF, R_P, R_M = range(3)

QUARTERS = [(q * CH, CH) for q in range(NQ)]
HALVES = [(0, 80), (80, 80)]
ROUTES = {
    "own_up": (UP, "x", 0, "x", 2, QUARTERS),
    "own_down": (DOWN, "x", 0, "x", 4, QUARTERS),
    "own_across": (ACROSS, "x", 0, "x", 7, QUARTERS),
    "far_up": (UP, "x", 2, "x", 1, QUARTERS[:2]),
    "far_down": (DOWN, "x", 4, "x", 1, QUARTERS[2:]),
    "far_across": (ACROSS, "x", 1, "x", 3, QUARTERS),
    "side_up": (UP, "x", 7, "x", 5, QUARTERS),
    "side_down": (DOWN, "x", 7, "x", 6, QUARTERS),
    "att_own": (ACROSS, "a", 7, "b", OWN, HALVES),
    "att_far": (ACROSS, "a", 3, "b", FAR, HALVES),
    "att_near_m": (ACROSS, "a", 5, "b", NEAR_M, HALVES),
    "att_near_p": (ACROSS, "a", 6, "b", NEAR_P, HALVES),
    "half_down": (DOWN, "p", FAR, "r", R_HALF, QUARTERS[:2]),
    "half_up": (UP, "p", FAR, "r", R_HALF, QUARTERS[2:]),
    "sum_down": (DOWN, "p", NEAR_M, "r", R_P, QUARTERS),
    "sum_up": (UP, "p", NEAR_P, "r", R_M, QUARTERS),
}
WEIGHTS = {
    "w_beyond": (BEYOND, True, 0, (0, 1, 2, 3)),
    "w_zup": (ZUP, False, 0, (0, 1, 2, 3)),
    "w_zdown": (ZDOWN, False, 0, (0, 1, 2, 3)),
    "w_fwd_up": (ZUP, False, 3, (0, 1)),
    "w_fwd_down": (ZDOWN, False, 1, (2, 3)),
    "w_core0": (CORE, False, 0, (None,)),
    "w_core3": (CORE, False, 3, (None,)),
    "w_core1": (CORE, False, 1, (None,)),
    "w_core2": (CORE, False, 2, (None,)),
}
BASE = {}
COUNT = 0
for _name, _spec in ROUTES.items():
    BASE[_name] = COUNT
    COUNT += len(_spec[5])
for _name, _spec in WEIGHTS.items():
    BASE[_name] = COUNT
    COUNT += len(_spec[3])
PIECE = QC // 8
SUB = PIECE // 4


def body(
    tokens_hbm, gain_hbm, wq_hbm, wk_hbm, wv_hbm, wo_hbm, kv_hbm, exps_hbm, cos_hbm, sin_hbm,
    pad_hbm, unpad_hbm, pad_k_hbm, pad_v_hbm, parity_hbm, out_hbm,
    xg, pb, rb, ab, bb, w_in, w_out, w_two, kv, raw, acc, qkv, qp, kp, vp, ap, exps, gains,
    gain_ref, exps_ref, cos_ref, sin_ref, pad_ref, unpad_ref, pad_k_ref, pad_v_ref, parity_ref,
    load_sem, send_sem, recv_sem, out_sem,
):
    me = lax.axis_index("tensor")
    mx, my = me // 4, me % 4
    dp = lax.axis_index("dp")
    hi, z, core = dp // 8, (dp // 2) % 4, dp % 2
    other = (1 - mx) * 4 + my
    z_next, z_last = (z + 1) % 4, (z + 3) % 4
    targets = {
        UP: {"tensor": mx * 4 + (my + 1) % 4},
        DOWN: {"tensor": mx * 4 + (my + 3) % 4},
        ACROSS: {"tensor": other},
        BEYOND: {"dp": (1 - hi) * 8 + z * 2 + core, "tensor": other},
        ZUP: {"dp": hi * 8 + z_next * 2 + core},
        ZDOWN: {"dp": hi * 8 + z_last * 2 + core},
        CORE: {"dp": hi * 8 + z * 2 + (1 - core)},
    }
    buffers = {"x": xg, "p": pb, "r": rb, "a": ab, "b": bb}

    def route(name, i):
        k = BASE[name] + i
        if name in ROUTES:
            target, sbuf, sslot, dbuf, dslot, pieces = ROUTES[name]
            at = pl.ds(*pieces[i])
            if sbuf == "a":
                src, dst = ab.at[sslot, at, :], bb.at[dslot, at, :]
            else:
                src, dst = buffers[sbuf].at[sslot, :, at], buffers[dbuf].at[dslot, :, at]
        else:
            target, mine, dz, subs = WEIGHTS[name]
            first = (((z + dz) % 4) * 2 + core) * PIECE
            if subs[i] is None:
                rows = pl.ds(pl.multiple_of(first, PIECE), PIECE)
            else:
                rows = pl.ds(pl.multiple_of(first + subs[i] * SUB, SUB), SUB)
            src, dst = (w_out if mine else w_two).at[rows, :], w_two.at[rows, :]
        return pltpu.make_async_remote_copy(
            src_ref=src, dst_ref=dst, send_sem=send_sem.at[k], recv_sem=recv_sem.at[k],
            device_id=targets[target], device_id_type=MESH,
        )

    def pieces_of(name, which):
        if which is not None:
            return which
        return range(len(ROUTES[name][5] if name in ROUTES else WEIGHTS[name][3]))

    def send(name, which=None):
        for i in pieces_of(name, which):
            route(name, i).start()

    def arrived(name, which=None):
        for i in pieces_of(name, which):
            received(name, i).wait_recv()

    def received(name, i):
        if name in ROUTES:
            return route(name, i)
        k = BASE[name] + i
        target, _, dz, subs = WEIGHTS[name]
        sender_z = {BEYOND: z, ZUP: z_last, ZDOWN: z_next, CORE: z}[target]
        sender_core = (1 - core) if target == CORE else core
        first = (((sender_z + dz) % 4) * 2 + sender_core) * PIECE
        if subs[i] is None:
            rows = pl.ds(pl.multiple_of(first, PIECE), PIECE)
        else:
            rows = pl.ds(pl.multiple_of(first + subs[i] * SUB, SUB), SUB)
        return pltpu.make_async_remote_copy(
            src_ref=w_two.at[rows, :], dst_ref=w_two.at[rows, :], send_sem=send_sem.at[k],
            recv_sem=recv_sem.at[k], device_id=targets[target], device_id_type=MESH,
        )

    def norm():
        def some(i5, c):
            squares = []
            for i in range(5):
                rows = pl.ds(pl.multiple_of((i5 * 5 + i) * 16, 16), 16)
                total = None
                for g in range(D // HD):
                    x = raw[rows, g * HD : (g + 1) * HD].astype(F32)
                    total = x * x if g == 0 else total + x * x
                squares.append(total)
            scales = [
                lax.rsqrt(jnp.sum(x, axis=-1, keepdims=True) * (1.0 / D) + EPS) for x in squares
            ]
            for i in range(5):
                rows = pl.ds(pl.multiple_of((i5 * 5 + i) * 16, 16), 16)
                xg[0, rows, :] = (raw[rows, :].astype(F32) * scales[i] * gains[...]).astype(BF16)
            return c

        lax.fori_loop(0, 2, some, 0)

    barrier = pltpu.get_barrier_semaphore()
    for target in targets.values():
        pl.semaphore_signal(barrier, inc=1, device_id=target, device_id_type=MESH)
    load_x = pltpu.make_async_copy(tokens_hbm, raw, load_sem.at[0])
    load_o = pltpu.make_async_copy(wo_hbm, w_out, load_sem.at[1])
    load_q = pltpu.make_async_copy(wq_hbm, w_in.at[:, pl.ds(0, QC)], load_sem.at[2])
    load_k = pltpu.make_async_copy(wk_hbm, w_in.at[:, pl.ds(QC, HD)], load_sem.at[3])
    load_v = pltpu.make_async_copy(wv_hbm, w_in.at[:, pl.ds(QC + HD, HD)], load_sem.at[4])
    load_kv = pltpu.make_async_copy(kv_hbm, kv, load_sem.at[5])
    small = [
        pltpu.make_async_copy(src, dst, load_sem.at[6 + i])
        for i, (src, dst) in enumerate((
            (gain_hbm, gain_ref), (exps_hbm, exps_ref), (cos_hbm, cos_ref), (sin_hbm, sin_ref),
            (pad_hbm, pad_ref), (unpad_hbm, unpad_ref), (pad_k_hbm, pad_k_ref),
            (pad_v_hbm, pad_v_ref), (parity_hbm, parity_ref),
        ))
    ]
    for copy in (small[0], load_x, load_o, *small[1:], load_q, load_k, load_v, load_kv):
        copy.start()
    small[0].wait()
    gain = gain_ref[...].astype(F32)
    for g in range(D // HD):
        gains[:, g * HD : (g + 1) * HD] = jnp.broadcast_to(gain[g : g + 1], (16, HD))
    load_x.wait()
    norm()
    pl.semaphore_wait(barrier, len(targets))

    for i in range(NQ):
        if i < 2:
            send("own_up", (i,))
            send("own_down", (i + 2,))
        if i < 3:
            send("own_across", (i,))
    load_o.wait()
    send("w_beyond")

    for copy in small[1:]:
        copy.wait()
    fill = jnp.zeros((HD - 32, HD), F32)
    for i in range(8 * ROWS_B // HD):
        at = slice(i * HD, (i + 1) * HD)
        exps[at, :] = jnp.concatenate([exps_ref[:, at].astype(F32), fill], 0).T

    def rot(m):
        return m * cos_ref[...] + pltpu.roll(m, HD // 2, 1) * sin_ref[...]

    def turn(m, n):
        second_head = rot(m[:, HD:]) if n < 4 else m[:, HD:]
        return jnp.concatenate([rot(m[:, :HD]), second_head], 1).astype(BF16)

    def project(j):
        for n in range(5):
            at = slice(n * 256, (n + 1) * 256)
            m = jnp.dot(xg[j], w_in[:, at], preferred_element_type=F32)
            qkv[0, :, at] = turn(m, n)

    early = 3 * CH

    def project_sides(first):
        for n in range(5):
            at = slice(n * 256, (n + 1) * 256)
            if first:
                rows = xg[5:7, :, :early].reshape(2 * ROWS_B, early)
                acc[:, at] = jnp.dot(rows, w_in[:early, at], preferred_element_type=F32)
            else:
                rows = xg[5:7, :, early:].reshape(2 * ROWS_B, D - early)
                m = acc[:, at] + jnp.dot(rows, w_in[early:, at], preferred_element_type=F32)
                for i in range(2):
                    qkv[i, :, at] = turn(m[i * ROWS_B : (i + 1) * ROWS_B], n)

    def spread_out(i):
        for n in range(4):
            at = slice(n * 256, (n + 1) * 256)
            qp[:, at] = jnp.dot(
                pad_ref[...], qkv[i, :, at], preferred_element_type=F32
            ).astype(BF16)
        kp[...] = jnp.dot(
            pad_k_ref[...], qkv[i, :, QC : QC + HD], preferred_element_type=F32
        ).astype(BF16)
        vp[...] = jnp.dot(
            pad_v_ref[...], qkv[i, :, QC + HD :], preferred_element_type=F32
        ).astype(BF16)

    def attend(j, t, half):
        lane = lax.broadcasted_iota(jnp.int32, (HD, HD), 1)
        token = lax.broadcasted_iota(jnp.int32, (HD, HD), 0) % 16
        seen = (lane % 2 == 0) | (lane <= 2 * token + 1)
        contract_last = (((1,), (1,)), ((), ()))
        batch = 4

        def some(s4, c):
            scores, values = [], []
            for i in range(batch):
                s = s4 * batch + i
                rows = pl.ds(pl.multiple_of(s * 16, 16), 16)
                spread = pl.ds(pl.multiple_of(s * 32, 32), 32)
                query = jnp.concatenate([qp[rows, h * HD : (h + 1) * HD] for h in range(HEADS)], 0)
                pairs = kv[t * SEQ_BLOCK + s]
                keys = jnp.concatenate([pairs[:32] * parity_ref[0] + kp[spread, :], pairs[32:]], 0)
                values.append(
                    jnp.concatenate([pairs[:32] * parity_ref[1] + vp[spread, :], pairs[32:]], 0)
                )
                scores.append(
                    lax.dot_general(query, keys, contract_last, preferred_element_type=F32)
                )
            scores = [jnp.where(seen, x, -1e30) for x in scores]
            tops = [jnp.max(x, axis=1, keepdims=True) for x in scores]
            raised = [jnp.exp2((x - top) * SCORE) for x, top in zip(scores, tops)]
            totals = [jnp.sum(x, axis=1, keepdims=True) for x in raised]
            probs = [(x * (1.0 / total)).astype(BF16) for x, total in zip(raised, totals)]
            for i in range(batch):
                rows = pl.ds(pl.multiple_of((s4 * batch + i) * 16, 16), 16)
                p = pltpu.roll(probs[i], 1, 1)
                att = jnp.dot(p, values[i], preferred_element_type=F32).astype(BF16)
                for h in range(HEADS):
                    ap[rows, h * HD : (h + 1) * HD] = att[h * 16 : (h + 1) * 16]
            return c

        parts = SEQ_BLOCK // batch // 2
        lax.fori_loop(half * parts, (half + 1) * parts, some, 0)
        rows = slice(half * 80, (half + 1) * 80)
        for n in range(4):
            at = slice(n * 256, (n + 1) * 256)
            padded = ap[half * 128 : (half + 1) * 128, at]
            ab[j, rows, at] = jnp.dot(
                unpad_ref[...], padded, preferred_element_type=F32
            ).astype(BF16)

    def powers(t, sign):
        e = exps[pl.ds(pl.multiple_of(t * ROWS_B, ROWS_B), ROWS_B), :].astype(jnp.int32)
        if sign < 0:
            return jnp.left_shift(1, -e).astype(F32)
        return jnp.left_shift(1, e + 11).astype(F32) * (2.0**-11)

    def out_project(att, weights, k, t, order, extra, done):
        shrink = powers(t, -1)
        for q in order:
            for base in (q * CH, q * CH + 512):
                part = jnp.dot(att, weights[:, base : base + 512], preferred_element_type=F32)
                for g in range(4):
                    at = slice(base + g * HD, base + (g + 1) * HD)
                    group = base // HD + g
                    scaled = part[:, g * HD : (g + 1) * HD] * shrink[:, group : group + 1]
                    scaled = jnp.clip(scaled, -127.0, 127.0).astype(BF16)
                    for r in extra(q, g == 0 and base == q * CH):
                        scaled = scaled.astype(F32) + r[:, at].astype(F32)
                    pb[k, :, at] = scaled.astype(BF16)
            done(q)

    def column_block(j):
        return j - j // 4

    def second(k, dy, order, half, name):
        t = mx * 4 + (my + dy) % 4

        def extra(q, first):
            refs = [pb.at[k]]
            if half is not None and q in half[1]:
                if first:
                    arrived(half[0], (half[1].index(q),))
                refs.append(rb.at[R_HALF])
            return refs

        def done(q):
            if name == "half":
                send("half_down" if q < 2 else "half_up", (q % 2,))
            elif name:
                send(name, (q,))

        out_project(bb[k], w_two, k, t, order, extra, done)

    def when(j, k, action):
        pl.when(j == k)(action)

    def before(j):
        @functools.partial(when, j, 1)
        def _():
            arrived("own_up", (0,))
            send("far_up", (0,))
            send("own_up", (2,))
            arrived("own_down", (2,))
            send("far_down", (0,))
            send("own_down", (0,))
            for i in range(4):
                arrived("w_beyond", (i,))
                send("w_zup", (i,))
                send("w_zdown", (i,))
                if i == 1:
                    arrived("own_up", (1,))
                    send("far_up", (1,))
                    send("own_up", (3,))
                    arrived("own_down", (3,))
                    send("far_down", (1,))
                    send("own_down", (1,))
            arrived("far_up", (0,))
            send("far_across", (0,))
            arrived("far_down", (0,))
            send("far_across", (2,))
            send("w_core0")
            arrived("own_across", (0, 1, 2))
            send("side_up", (0, 1, 2))
            send("side_down", (0, 1, 2))
            arrived("w_zup", (0, 1))
            send("w_fwd_up")
            arrived("w_zdown", (2, 3))
            send("w_fwd_down")
            arrived("far_up", (1,))
            send("far_across", (1,))
            arrived("far_down", (1,))
            send("far_across", (3,))
            send("own_across", (3,))

        @functools.partial(when, j, 2)
        def _():
            arrived("w_zup", (2, 3))
            send("w_core3")
            arrived("w_zdown", (0, 1))
            send("w_core1")
            arrived("own_up", (2, 3))

        @functools.partial(when, j, 3)
        def _():
            arrived("w_fwd_up")
            arrived("w_fwd_down")
            send("w_core2")
            arrived("far_across")

        @functools.partial(when, j, 4)
        def _():
            arrived("own_down", (0, 1))
            arrived("own_across", (3,))
            send("side_up", (3,))
            send("side_down", (3,))

        @functools.partial(when, j, 5)
        def _():
            for name in ("w_core0", "w_core3", "w_core1", "w_core2"):
                arrived(name)
            arrived("att_far")
            second(FAR, 2, (0, 2, 1, 3), None, "half")
            arrived("side_up", (0, 1, 2))
            arrived("side_down", (0, 1, 2))
            project_sides(True)
            arrived("side_up", (3,))
            arrived("side_down", (3,))
            project_sides(False)

        @functools.partial(when, j, 7)
        def _():
            arrived("att_near_m")
            second(NEAR_M, 3, (2, 3, 0, 1), ("half_down", (0, 1)), "sum_down")
            arrived("att_near_p")
            second(NEAR_P, 1, (0, 1, 2, 3), ("half_up", (2, 3)), "sum_up")

    def step(j, c):
        dx = (DX_BITS >> j) & 1
        dy = (DY_BITS >> (2 * j)) & 3
        t = ((mx + dx) % 2) * 4 + (my + dy) % 4
        before(j)

        @pl.when((j < 5) | (j == 7))
        def _():
            project(j)

        spread_out(j // 6 - j // 7)
        for half in range(2):
            attend(j, t, half)
            for slot, name in (
                (3, "att_far"), (5, "att_near_m"), (6, "att_near_p"), (7, "att_own"),
            ):
                when(j, slot, functools.partial(send, name, (half,)))

        @pl.when(dx == 0)
        def _():
            out_project(
                ab[j], w_out, column_block(j), t, range(NQ), lambda q, first: (), lambda q: None
            )

        return c

    load_q.wait()
    load_k.wait()
    load_v.wait()
    load_kv.wait()
    lax.fori_loop(0, 8, step, 0)

    arrived("att_own")
    second(OWN, 0, range(NQ), None, None)

    restore = powers(me, 1)
    outs = []
    for q in (0, 2, 1, 3):
        arrived("sum_down", (q,))
        arrived("sum_up", (q,))
        for g in range(CH // HD):
            group = q * (CH // HD) + g
            at = slice(group * HD, (group + 1) * HD)
            total = pb[OWN, :, at].astype(F32)
            for r in (R_P, R_M):
                total = total + rb[r, :, at].astype(F32)
            mixed = raw[:, at].astype(F32) + total * restore[:, group : group + 1]
            raw[:, at] = mixed.astype(BF16)
        at = pl.ds(*QUARTERS[q])
        copy = pltpu.make_async_copy(raw.at[:, at], out_hbm.at[:, at], out_sem.at[q])
        copy.start()
        outs.append(copy)
    for copy in outs:
        copy.wait()
    for name in (*ROUTES, *WEIGHTS):
        for i in pieces_of(name, None):
            route(name, i).wait_send()


def tables():
    position = (np.arange(ROWS_B) % NEW + CACHE).astype(np.float32)
    frequency = THETA ** (-(np.arange(HD // 2, dtype=np.float32) * np.float32(2.0)) / np.float32(HD))
    angles = position[:, None] * frequency.astype(np.float32)[None, :]
    cosine, sine = np.cos(angles), np.sin(angles)
    row = np.arange(ROWS_B)
    spread = np.zeros((PADDED, ROWS_B), np.float32)
    spread[row // NEW * 16 + row % NEW, row] = 1.0
    keys = np.zeros((SPREAD, ROWS_B), np.float32)
    keys[row // NEW * 32 + 2 * (row % NEW) + 1, row] = 1.0
    values = np.zeros((SPREAD, ROWS_B), np.float32)
    values[row // NEW * 32 + 2 * (row % NEW) + 2, row] = 1.0
    even = np.broadcast_to((np.arange(32) % 2 == 0)[:, None], (32, HD))
    return (
        jnp.asarray(np.concatenate([cosine, cosine], 1), F32),
        jnp.asarray(np.concatenate([-sine, sine], 1), F32),
        jnp.asarray(spread, BF16),
        jnp.asarray(spread.T[: ROWS_B // 2, : PADDED // 2], BF16),
        jnp.asarray(keys, BF16),
        jnp.asarray(values, BF16),
        jnp.asarray(np.stack([even, ~even]), BF16),
    )


def on_device(
    tokens, norm_gain, query_weight, key_weight, value_weight, out_weight, past_cache, exponents
):
    seqs = past_cache.shape[0]
    pairs = past_cache.reshape(seqs, 2 * CACHE, HD)
    anywhere = pl.BlockSpec(memory_space=pl.ANY)
    return pl.pallas_call(
        body,
        out_shape=jax.ShapeDtypeStruct(tokens.shape, BF16),
        in_specs=[anywhere] * 15,
        out_specs=anywhere,
        scratch_shapes=[
            pltpu.VMEM((8, ROWS_B, D), BF16),
            pltpu.VMEM((4, ROWS_B, D), BF16),
            pltpu.VMEM((3, ROWS_B, D), BF16),
            pltpu.VMEM((8, ROWS_B, QC), BF16),
            pltpu.VMEM((4, ROWS_B, QC), BF16),
            pltpu.VMEM((D, QC + 2 * HD), BF16),
            pltpu.VMEM((QC, D), BF16),
            pltpu.VMEM((QC, D), BF16),
            pltpu.VMEM((seqs, 2 * CACHE, HD), BF16),
            pltpu.VMEM((ROWS_B, D), BF16),
            pltpu.VMEM((2 * ROWS_B, QC + 2 * HD), F32),
            pltpu.VMEM((2, ROWS_B, QC + 2 * HD), BF16),
            pltpu.VMEM((PADDED, QC), BF16),
            pltpu.VMEM((SPREAD, HD), BF16),
            pltpu.VMEM((SPREAD, HD), BF16),
            pltpu.VMEM((PADDED, QC), BF16),
            pltpu.VMEM((8 * ROWS_B, HD), F32),
            pltpu.VMEM((16, D), F32),
            pltpu.VMEM((D // HD, HD), BF16),
            pltpu.VMEM((D // HD, exponents.shape[0]), jnp.int32),
            pltpu.VMEM((ROWS_B, HD), F32),
            pltpu.VMEM((ROWS_B, HD), F32),
            pltpu.VMEM((PADDED, ROWS_B), BF16),
            pltpu.VMEM((ROWS_B // 2, PADDED // 2), BF16),
            pltpu.VMEM((SPREAD, ROWS_B), BF16),
            pltpu.VMEM((SPREAD, ROWS_B), BF16),
            pltpu.VMEM((2, 32, HD), BF16),
            pltpu.SemaphoreType.DMA((15,)),
            pltpu.SemaphoreType.DMA((COUNT,)),
            pltpu.SemaphoreType.DMA((COUNT,)),
            pltpu.SemaphoreType.DMA((NQ,)),
        ],
        compiler_params=pltpu.CompilerParams(
            collective_id=0, has_side_effects=True, vmem_limit_bytes=67_000_000
        ),
        name="verify_block",
    )(
        tokens, norm_gain.reshape(D // HD, HD), query_weight, key_weight, value_weight, out_weight,
        pairs, exponents.T, *tables(),
    )


def solution(mesh):
    return jax.shard_map(
        on_device,
        mesh=mesh,
        in_specs=(
            P(("dp", "tensor"), None),
            P(),
            P(None, "tensor"),
            P(None, "tensor"),
            P(None, "tensor"),
            P("tensor", None),
            P("dp", None, None, "tensor"),
            P("dp", None),
        ),
        out_specs=P(("dp", "tensor"), None),
        check_vma=False,
    )
```

```python
import functools

import jax
import jax.numpy as jnp
import numpy as np
from jax import lax
from jax.experimental import pallas as pl
from jax.experimental.pallas import tpu as pltpu
from jax.sharding import PartitionSpec as P

HD = 128
NEW = 10
CACHE = 64
D = 4096
HEADS = 8
QC = 1024
SEQ_BLOCK = 16
ROWS_B = 160
PADDED = 256
SPREAD = 512
CH = 1024
NQ = 4
EPS = 1e-05
THETA = 500000.0
MESH = pl.DeviceIdType.MESH
F32 = jnp.float32
BF16 = jnp.bfloat16
SCORE = float(np.log2(np.e) / np.sqrt(HD))

SLOTS = ((0, 0), (0, 2), (0, 3), (1, 2), (0, 1), (1, 3), (1, 1), (1, 0))
DX_BITS = sum(dx << j for j, (dx, _) in enumerate(SLOTS))
DY_BITS = sum(dy << (2 * j) for j, (_, dy) in enumerate(SLOTS))

UP, DOWN, ACROSS, BEYOND, ZUP, ZDOWN, CORE = range(7)
OWN, FAR, NEAR_M, NEAR_P = range(4)
R_HALF, R_P, R_M = range(3)

QUARTERS = [(q * CH, CH) for q in range(NQ)]
HALF = ROWS_B // 2
HALVES = [(0, HALF), (HALF, HALF)]
EIGHTHS = [(q * CH, CH, r * HALF, HALF) for r in range(2) for q in range(NQ)]
ROUTES = {
    "own_up": (UP, "x", 0, "x", 2, QUARTERS),
    "own_down": (DOWN, "x", 0, "x", 4, QUARTERS),
    "own_across": (ACROSS, "x", 0, "x", 7, QUARTERS),
    "far_up": (UP, "x", 2, "x", 1, QUARTERS[:2]),
    "far_down": (DOWN, "x", 4, "x", 1, QUARTERS[2:]),
    "far_across": (ACROSS, "x", 1, "x", 3, QUARTERS),
    "side_up": (UP, "x", 7, "x", 5, QUARTERS),
    "side_down": (DOWN, "x", 7, "x", 6, QUARTERS),
    "att_own": (ACROSS, "a", 7, "b", OWN, HALVES),
    "att_far": (ACROSS, "a", 3, "b", FAR, HALVES),
    "att_near_m": (ACROSS, "a", 5, "b", NEAR_M, HALVES),
    "att_near_p": (ACROSS, "a", 6, "b", NEAR_P, HALVES),
    "half_down": (DOWN, "p", FAR, "r", R_HALF, QUARTERS[:2]),
    "half_up": (UP, "p", FAR, "r", R_HALF, QUARTERS[2:]),
    "sum_down": (DOWN, "p", NEAR_M, "r", R_P, EIGHTHS),
    "sum_up": (UP, "p", NEAR_P, "r", R_M, EIGHTHS),
}
WEIGHTS = {
    "w_beyond": (BEYOND, True, 0, (0, 1, 2, 3)),
    "w_zup": (ZUP, False, 0, (0, 1, 2, 3)),
    "w_zdown": (ZDOWN, False, 0, (0, 1, 2, 3)),
    "w_fwd_up": (ZUP, False, 3, (0, 1)),
    "w_fwd_down": (ZDOWN, False, 1, (2, 3)),
    "w_core0": (CORE, False, 0, (None,)),
    "w_core3": (CORE, False, 3, (None,)),
    "w_core1": (CORE, False, 1, (None,)),
    "w_core2": (CORE, False, 2, (None,)),
}
BASE = {}
COUNT = 0
for _name, _spec in ROUTES.items():
    BASE[_name] = COUNT
    COUNT += len(_spec[5])
for _name, _spec in WEIGHTS.items():
    BASE[_name] = COUNT
    COUNT += len(_spec[3])
PIECE = QC // 8
SUB = PIECE // 4


def body(
    tokens_hbm, gain_hbm, wq_hbm, wk_hbm, wv_hbm, wo_hbm, kv_hbm, exps_hbm, cos_hbm, sin_hbm,
    pad_hbm, unpad_hbm, pad_k_hbm, pad_v_hbm, parity_hbm, out_hbm,
    xg, pb, rb, ab, bb, w_in, w_out, w_two, kv, raw, acc, qkv, qp, kp, vp, ap, exps, gains,
    gain_ref, exps_ref, cos_ref, sin_ref, pad_ref, unpad_ref, pad_k_ref, pad_v_ref, parity_ref,
    load_sem, send_sem, recv_sem, out_sem,
):
    me = lax.axis_index("tensor")
    mx, my = me // 4, me % 4
    dp = lax.axis_index("dp")
    hi, z, core = dp // 8, (dp // 2) % 4, dp % 2
    other = (1 - mx) * 4 + my
    z_next, z_last = (z + 1) % 4, (z + 3) % 4
    targets = {
        UP: {"tensor": mx * 4 + (my + 1) % 4},
        DOWN: {"tensor": mx * 4 + (my + 3) % 4},
        ACROSS: {"tensor": other},
        BEYOND: {"dp": (1 - hi) * 8 + z * 2 + core, "tensor": other},
        ZUP: {"dp": hi * 8 + z_next * 2 + core},
        ZDOWN: {"dp": hi * 8 + z_last * 2 + core},
        CORE: {"dp": hi * 8 + z * 2 + (1 - core)},
    }
    buffers = {"x": xg, "p": pb, "r": rb, "a": ab, "b": bb}

    def route(name, i):
        k = BASE[name] + i
        if name in ROUTES:
            target, sbuf, sslot, dbuf, dslot, pieces = ROUTES[name]
            at = pl.ds(*pieces[i][:2])
            if len(pieces[i]) == 4:
                rows = pl.ds(*pieces[i][2:])
                src, dst = buffers[sbuf].at[sslot, rows, at], buffers[dbuf].at[dslot, rows, at]
            elif sbuf == "a":
                src, dst = ab.at[sslot, at, :], bb.at[dslot, at, :]
            else:
                src, dst = buffers[sbuf].at[sslot, :, at], buffers[dbuf].at[dslot, :, at]
        else:
            target, mine, dz, subs = WEIGHTS[name]
            first = (((z + dz) % 4) * 2 + core) * PIECE
            if subs[i] is None:
                rows = pl.ds(pl.multiple_of(first, PIECE), PIECE)
            else:
                rows = pl.ds(pl.multiple_of(first + subs[i] * SUB, SUB), SUB)
            src, dst = (w_out if mine else w_two).at[rows, :], w_two.at[rows, :]
        return pltpu.make_async_remote_copy(
            src_ref=src, dst_ref=dst, send_sem=send_sem.at[k], recv_sem=recv_sem.at[k],
            device_id=targets[target], device_id_type=MESH,
        )

    def pieces_of(name, which):
        if which is not None:
            return which
        return range(len(ROUTES[name][5] if name in ROUTES else WEIGHTS[name][3]))

    def send(name, which=None):
        for i in pieces_of(name, which):
            route(name, i).start()

    def arrived(name, which=None):
        for i in pieces_of(name, which):
            received(name, i).wait_recv()

    def received(name, i):
        if name in ROUTES:
            return route(name, i)
        k = BASE[name] + i
        target, _, dz, subs = WEIGHTS[name]
        sender_z = {BEYOND: z, ZUP: z_last, ZDOWN: z_next, CORE: z}[target]
        sender_core = (1 - core) if target == CORE else core
        first = (((sender_z + dz) % 4) * 2 + sender_core) * PIECE
        if subs[i] is None:
            rows = pl.ds(pl.multiple_of(first, PIECE), PIECE)
        else:
            rows = pl.ds(pl.multiple_of(first + subs[i] * SUB, SUB), SUB)
        return pltpu.make_async_remote_copy(
            src_ref=w_two.at[rows, :], dst_ref=w_two.at[rows, :], send_sem=send_sem.at[k],
            recv_sem=recv_sem.at[k], device_id=targets[target], device_id_type=MESH,
        )

    def norm():
        def some(i5, c):
            squares = []
            for i in range(5):
                rows = pl.ds(pl.multiple_of((i5 * 5 + i) * 16, 16), 16)
                total = None
                for g in range(D // HD):
                    x = raw[rows, g * HD : (g + 1) * HD].astype(F32)
                    total = x * x if g == 0 else total + x * x
                squares.append(total)
            scales = [
                lax.rsqrt(jnp.sum(x, axis=-1, keepdims=True) * (1.0 / D) + EPS) for x in squares
            ]
            for i in range(5):
                rows = pl.ds(pl.multiple_of((i5 * 5 + i) * 16, 16), 16)
                xg[0, rows, :] = (raw[rows, :].astype(F32) * scales[i] * gains[...]).astype(BF16)
            return c

        lax.fori_loop(0, 2, some, 0)

    barrier = pltpu.get_barrier_semaphore()
    for target in targets.values():
        pl.semaphore_signal(barrier, inc=1, device_id=target, device_id_type=MESH)
    load_x = pltpu.make_async_copy(tokens_hbm, raw, load_sem.at[0])
    load_o = pltpu.make_async_copy(wo_hbm, w_out, load_sem.at[1])
    load_q = pltpu.make_async_copy(wq_hbm, w_in.at[:, pl.ds(0, QC)], load_sem.at[2])
    load_k = pltpu.make_async_copy(wk_hbm, w_in.at[:, pl.ds(QC, HD)], load_sem.at[3])
    load_v = pltpu.make_async_copy(wv_hbm, w_in.at[:, pl.ds(QC + HD, HD)], load_sem.at[4])
    load_kv = pltpu.make_async_copy(kv_hbm, kv, load_sem.at[5])
    small = [
        pltpu.make_async_copy(src, dst, load_sem.at[6 + i])
        for i, (src, dst) in enumerate((
            (gain_hbm, gain_ref), (exps_hbm, exps_ref), (cos_hbm, cos_ref), (sin_hbm, sin_ref),
            (pad_hbm, pad_ref), (unpad_hbm, unpad_ref), (pad_k_hbm, pad_k_ref),
            (pad_v_hbm, pad_v_ref), (parity_hbm, parity_ref),
        ))
    ]
    for copy in (small[0], load_x, load_o, *small[1:], load_q, load_k, load_v, load_kv):
        copy.start()
    small[0].wait()
    gain = gain_ref[...].astype(F32)
    for g in range(D // HD):
        gains[:, g * HD : (g + 1) * HD] = jnp.broadcast_to(gain[g : g + 1], (16, HD))
    load_x.wait()
    norm()
    pl.semaphore_wait(barrier, len(targets))

    for i in range(NQ):
        if i < 2:
            send("own_up", (i,))
            send("own_down", (i + 2,))
        if i < 3:
            send("own_across", (i,))
    load_o.wait()
    send("w_beyond")

    for copy in small[1:]:
        copy.wait()
    fill = jnp.zeros((HD - 32, HD), F32)
    for i in range(8 * ROWS_B // HD):
        at = slice(i * HD, (i + 1) * HD)
        exps[at, :] = jnp.concatenate([exps_ref[:, at].astype(F32), fill], 0).T

    def rot(m):
        return m * cos_ref[...] + pltpu.roll(m, HD // 2, 1) * sin_ref[...]

    def turn(m, n):
        second_head = rot(m[:, HD:]) if n < 4 else m[:, HD:]
        return jnp.concatenate([rot(m[:, :HD]), second_head], 1).astype(BF16)

    def project(j):
        for n in range(5):
            at = slice(n * 256, (n + 1) * 256)
            m = jnp.dot(xg[j], w_in[:, at], preferred_element_type=F32)
            qkv[0, :, at] = turn(m, n)

    early = 3 * CH

    def project_sides(first):
        for n in range(5):
            at = slice(n * 256, (n + 1) * 256)
            if first:
                rows = xg[5:7, :, :early].reshape(2 * ROWS_B, early)
                acc[:, at] = jnp.dot(rows, w_in[:early, at], preferred_element_type=F32)
            else:
                rows = xg[5:7, :, early:].reshape(2 * ROWS_B, D - early)
                m = acc[:, at] + jnp.dot(rows, w_in[early:, at], preferred_element_type=F32)
                for i in range(2):
                    qkv[i, :, at] = turn(m[i * ROWS_B : (i + 1) * ROWS_B], n)

    def spread_out(i):
        for n in range(4):
            at = slice(n * 256, (n + 1) * 256)
            qp[:, at] = jnp.dot(
                pad_ref[...], qkv[i, :, at], preferred_element_type=F32
            ).astype(BF16)
        kp[...] = jnp.dot(
            pad_k_ref[...], qkv[i, :, QC : QC + HD], preferred_element_type=F32
        ).astype(BF16)
        vp[...] = jnp.dot(
            pad_v_ref[...], qkv[i, :, QC + HD :], preferred_element_type=F32
        ).astype(BF16)

    def attend(j, t, half):
        lane = lax.broadcasted_iota(jnp.int32, (HD, HD), 1)
        token = lax.broadcasted_iota(jnp.int32, (HD, HD), 0) % 16
        seen = (lane % 2 == 0) | (lane <= 2 * token + 1)
        contract_last = (((1,), (1,)), ((), ()))
        batch = 4

        def some(s4, c):
            scores, values = [], []
            for i in range(batch):
                s = s4 * batch + i
                rows = pl.ds(pl.multiple_of(s * 16, 16), 16)
                spread = pl.ds(pl.multiple_of(s * 32, 32), 32)
                query = jnp.concatenate([qp[rows, h * HD : (h + 1) * HD] for h in range(HEADS)], 0)
                pairs = kv[t * SEQ_BLOCK + s]
                keys = jnp.concatenate([pairs[:32] * parity_ref[0] + kp[spread, :], pairs[32:]], 0)
                values.append(
                    jnp.concatenate([pairs[:32] * parity_ref[1] + vp[spread, :], pairs[32:]], 0)
                )
                scores.append(
                    lax.dot_general(query, keys, contract_last, preferred_element_type=F32)
                )
            scores = [jnp.where(seen, x, -1e30) for x in scores]
            tops = [jnp.max(x, axis=1, keepdims=True) for x in scores]
            raised = [jnp.exp2((x - top) * SCORE) for x, top in zip(scores, tops)]
            totals = [jnp.sum(x, axis=1, keepdims=True) for x in raised]
            probs = [(x * (1.0 / total)).astype(BF16) for x, total in zip(raised, totals)]
            for i in range(batch):
                rows = pl.ds(pl.multiple_of((s4 * batch + i) * 16, 16), 16)
                p = pltpu.roll(probs[i], 1, 1)
                att = jnp.dot(p, values[i], preferred_element_type=F32).astype(BF16)
                for h in range(HEADS):
                    ap[rows, h * HD : (h + 1) * HD] = att[h * 16 : (h + 1) * 16]
            return c

        parts = SEQ_BLOCK // batch // 2
        lax.fori_loop(half * parts, (half + 1) * parts, some, 0)
        rows = slice(half * 80, (half + 1) * 80)
        for n in range(4):
            at = slice(n * 256, (n + 1) * 256)
            padded = ap[half * 128 : (half + 1) * 128, at]
            ab[j, rows, at] = jnp.dot(
                unpad_ref[...], padded, preferred_element_type=F32
            ).astype(BF16)

    def powers(t, sign, first=0, count=ROWS_B):
        e = exps[pl.ds(pl.multiple_of(t * ROWS_B + first, 16), count), :].astype(jnp.int32)
        if sign < 0:
            return jnp.left_shift(1, -e).astype(F32)
        return jnp.left_shift(1, e + 11).astype(F32) * (2.0**-11)

    def out_project(att, weights, k, t, order, extra, done, first=0, count=ROWS_B):
        shrink = powers(t, -1, first, count)
        rows = slice(first, first + count)
        for q in order:
            for base in (q * CH, q * CH + 512):
                part = jnp.dot(att, weights[:, base : base + 512], preferred_element_type=F32)
                for g in range(4):
                    at = slice(base + g * HD, base + (g + 1) * HD)
                    group = base // HD + g
                    scaled = part[:, g * HD : (g + 1) * HD] * shrink[:, group : group + 1]
                    scaled = jnp.clip(scaled, -127.0, 127.0).astype(BF16)
                    for r in extra(q, g == 0 and base == q * CH):
                        scaled = scaled.astype(F32) + r[rows, at].astype(F32)
                    pb[k, rows, at] = scaled.astype(BF16)
            done(q)

    def column_block(j):
        return j - j // 4

    def second(k, dy, order, send_sum, half=None, part=None):
        first, count = HALVES[part] if part is not None else (0, ROWS_B)

        def extra(q, opening):
            refs = [pb.at[k]]
            if half is not None and q in half[1]:
                if opening and part == 0:
                    arrived(half[0], (half[1].index(q),))
                refs.append(rb.at[R_HALF])
            return refs

        out_project(
            bb[k, first : first + count], w_two, k, mx * 4 + (my + dy) % 4, order, extra, send_sum,
            first, count,
        )

    def near(up, part, order):
        name = "sum_up" if up else "sum_down"

        def send_sum(q):
            send(name, (part * NQ + q,))

        if up:
            second(NEAR_P, 1, order, send_sum, ("half_up", (2, 3)), part)
        else:
            second(NEAR_M, 3, order, send_sum, ("half_down", (0, 1)), part)

    def when(j, k, action):
        pl.when(j == k)(action)

    def before(j):
        @functools.partial(when, j, 1)
        def _():
            arrived("own_up", (0,))
            send("far_up", (0,))
            send("own_up", (2,))
            arrived("own_down", (2,))
            send("far_down", (0,))
            send("own_down", (0,))
            for i in range(4):
                arrived("w_beyond", (i,))
                send("w_zup", (i,))
                send("w_zdown", (i,))
                if i == 1:
                    arrived("own_up", (1,))
                    send("far_up", (1,))
                    send("own_up", (3,))
                    arrived("own_down", (3,))
                    send("far_down", (1,))
                    send("own_down", (1,))
            arrived("far_up", (0,))
            send("far_across", (0,))
            arrived("far_down", (0,))
            send("far_across", (2,))
            send("w_core0")
            arrived("own_across", (0, 1, 2))
            send("side_up", (0, 1, 2))
            send("side_down", (0, 1, 2))
            arrived("w_zup", (0, 1))
            send("w_fwd_up")
            arrived("w_zdown", (2, 3))
            send("w_fwd_down")
            arrived("far_up", (1,))
            send("far_across", (1,))
            arrived("far_down", (1,))
            send("far_across", (3,))
            send("own_across", (3,))

        @functools.partial(when, j, 2)
        def _():
            arrived("w_zup", (2, 3))
            send("w_core3")
            arrived("w_zdown", (0, 1))
            send("w_core1")
            arrived("own_up", (2, 3))

        @functools.partial(when, j, 3)
        def _():
            arrived("w_fwd_up")
            arrived("w_fwd_down")
            send("w_core2")
            arrived("far_across")

        @functools.partial(when, j, 4)
        def _():
            arrived("own_down", (0, 1))
            arrived("own_across", (3,))
            send("side_up", (3,))
            send("side_down", (3,))

        @functools.partial(when, j, 5)
        def _():
            for name in ("w_core0", "w_core3", "w_core1", "w_core2"):
                arrived(name)
            arrived("att_far")
            second(FAR, 2, (0, 2, 1, 3), lambda q: send("half_down" if q < 2 else "half_up", (q % 2,)))
            arrived("side_up", (0, 1, 2))
            arrived("side_down", (0, 1, 2))
            project_sides(True)
            arrived("side_up", (3,))
            arrived("side_down", (3,))
            project_sides(False)

        @functools.partial(when, j, 7)
        def _():
            arrived("att_near_m", (0,))
            near(False, 0, (2, 3))
            arrived("att_near_p", (0,))
            near(True, 0, (0, 1))
            near(False, 0, (0, 1))
            near(True, 0, (2, 3))
            arrived("att_near_m", (1,))
            near(False, 1, (2, 3, 0, 1))
            arrived("att_near_p", (1,))
            near(True, 1, (0, 1, 2, 3))

    def step(j, c):
        dx = (DX_BITS >> j) & 1
        dy = (DY_BITS >> (2 * j)) & 3
        t = ((mx + dx) % 2) * 4 + (my + dy) % 4
        before(j)

        @pl.when((j < 5) | (j == 7))
        def _():
            project(j)

        spread_out(j // 6 - j // 7)
        for half in range(2):
            attend(j, t, half)
            when(j, 3, functools.partial(send, "att_far", (half,)))
            when(j, 7, functools.partial(send, "att_own", (half,)))
            if half == 0:
                when(j, 5, functools.partial(send, "att_near_m", (0,)))
            when(j, 6, functools.partial(send, "att_near_p", (half,)))
            if half == 0:
                when(j, 6, functools.partial(send, "att_near_m", (1,)))

        @pl.when(dx == 0)
        def _():
            out_project(
                ab[j], w_out, column_block(j), t, range(NQ), lambda q, first: (), lambda q: None
            )

        return c

    load_q.wait()
    load_k.wait()
    load_v.wait()
    load_kv.wait()
    lax.fori_loop(0, 8, step, 0)

    arrived("att_own")
    second(OWN, 0, range(NQ), lambda q: None)

    restore = powers(me, 1)
    outs = []
    for part in range(2):
        rows = slice(part * HALF, (part + 1) * HALF)
        for q in (0, 2, 1, 3):
            arrived("sum_down", (part * NQ + q,))
            arrived("sum_up", (part * NQ + q,))
            for g in range(CH // HD):
                group = q * (CH // HD) + g
                at = slice(group * HD, (group + 1) * HD)
                total = pb[OWN, rows, at].astype(F32)
                for r in (R_P, R_M):
                    total = total + rb[r, rows, at].astype(F32)
                mixed = raw[rows, at].astype(F32) + total * restore[rows, group : group + 1]
                raw[rows, at] = mixed.astype(BF16)
            tile = (pl.ds(*HALVES[part]), pl.ds(*QUARTERS[q]))
            copy = pltpu.make_async_copy(raw.at[tile], out_hbm.at[tile], out_sem.at[part * NQ + q])
            copy.start()
            outs.append(copy)
    for copy in outs:
        copy.wait()
    for name in (*ROUTES, *WEIGHTS):
        for i in pieces_of(name, None):
            route(name, i).wait_send()


def tables():
    position = (np.arange(ROWS_B) % NEW + CACHE).astype(np.float32)
    frequency = THETA ** (-(np.arange(HD // 2, dtype=np.float32) * np.float32(2.0)) / np.float32(HD))
    angles = position[:, None] * frequency.astype(np.float32)[None, :]
    cosine, sine = np.cos(angles), np.sin(angles)
    row = np.arange(ROWS_B)
    spread = np.zeros((PADDED, ROWS_B), np.float32)
    spread[row // NEW * 16 + row % NEW, row] = 1.0
    keys = np.zeros((SPREAD, ROWS_B), np.float32)
    keys[row // NEW * 32 + 2 * (row % NEW) + 1, row] = 1.0
    values = np.zeros((SPREAD, ROWS_B), np.float32)
    values[row // NEW * 32 + 2 * (row % NEW) + 2, row] = 1.0
    even = np.broadcast_to((np.arange(32) % 2 == 0)[:, None], (32, HD))
    return (
        jnp.asarray(np.concatenate([cosine, cosine], 1), F32),
        jnp.asarray(np.concatenate([-sine, sine], 1), F32),
        jnp.asarray(spread, BF16),
        jnp.asarray(spread.T[: ROWS_B // 2, : PADDED // 2], BF16),
        jnp.asarray(keys, BF16),
        jnp.asarray(values, BF16),
        jnp.asarray(np.stack([even, ~even]), BF16),
    )


def on_device(
    tokens, norm_gain, query_weight, key_weight, value_weight, out_weight, past_cache, exponents
):
    seqs = past_cache.shape[0]
    pairs = past_cache.reshape(seqs, 2 * CACHE, HD)
    anywhere = pl.BlockSpec(memory_space=pl.ANY)
    return pl.pallas_call(
        body,
        out_shape=jax.ShapeDtypeStruct(tokens.shape, BF16),
        in_specs=[anywhere] * 15,
        out_specs=anywhere,
        scratch_shapes=[
            pltpu.VMEM((8, ROWS_B, D), BF16),
            pltpu.VMEM((4, ROWS_B, D), BF16),
            pltpu.VMEM((3, ROWS_B, D), BF16),
            pltpu.VMEM((8, ROWS_B, QC), BF16),
            pltpu.VMEM((4, ROWS_B, QC), BF16),
            pltpu.VMEM((D, QC + 2 * HD), BF16),
            pltpu.VMEM((QC, D), BF16),
            pltpu.VMEM((QC, D), BF16),
            pltpu.VMEM((seqs, 2 * CACHE, HD), BF16),
            pltpu.VMEM((ROWS_B, D), BF16),
            pltpu.VMEM((2 * ROWS_B, QC + 2 * HD), F32),
            pltpu.VMEM((2, ROWS_B, QC + 2 * HD), BF16),
            pltpu.VMEM((PADDED, QC), BF16),
            pltpu.VMEM((SPREAD, HD), BF16),
            pltpu.VMEM((SPREAD, HD), BF16),
            pltpu.VMEM((PADDED, QC), BF16),
            pltpu.VMEM((8 * ROWS_B, HD), F32),
            pltpu.VMEM((16, D), F32),
            pltpu.VMEM((D // HD, HD), BF16),
            pltpu.VMEM((D // HD, exponents.shape[0]), jnp.int32),
            pltpu.VMEM((ROWS_B, HD), F32),
            pltpu.VMEM((ROWS_B, HD), F32),
            pltpu.VMEM((PADDED, ROWS_B), BF16),
            pltpu.VMEM((ROWS_B // 2, PADDED // 2), BF16),
            pltpu.VMEM((SPREAD, ROWS_B), BF16),
            pltpu.VMEM((SPREAD, ROWS_B), BF16),
            pltpu.VMEM((2, 32, HD), BF16),
            pltpu.SemaphoreType.DMA((15,)),
            pltpu.SemaphoreType.DMA((COUNT,)),
            pltpu.SemaphoreType.DMA((COUNT,)),
            pltpu.SemaphoreType.DMA((2 * NQ,)),
        ],
        compiler_params=pltpu.CompilerParams(
            collective_id=0, has_side_effects=True, vmem_limit_bytes=67_000_000
        ),
        name="verify_block",
    )(
        tokens, norm_gain.reshape(D // HD, HD), query_weight, key_weight, value_weight, out_weight,
        pairs, exponents.T, *tables(),
    )


def solution(mesh):
    return jax.shard_map(
        on_device,
        mesh=mesh,
        in_specs=(
            P(("dp", "tensor"), None),
            P(),
            P(None, "tensor"),
            P(None, "tensor"),
            P(None, "tensor"),
            P("tensor", None),
            P("dp", None, None, "tensor"),
            P("dp", None),
        ),
        out_specs=P(("dp", "tensor"), None),
        check_vma=False,
    )
```

```python
import functools

import jax
import jax.numpy as jnp
import numpy as np
from jax import lax
from jax.experimental import pallas as pl
from jax.experimental.pallas import tpu as pltpu
from jax.sharding import PartitionSpec as P

HD = 128
NEW = 10
CACHE = 64
D = 4096
HEADS = 8
QC = 1024
SEQ_BLOCK = 16
ROWS_B = 160
PADDED = 256
SPREAD = 512
CH = 1024
NQ = 4
EPS = 1e-05
THETA = 500000.0
MESH = pl.DeviceIdType.MESH
F32 = jnp.float32
BF16 = jnp.bfloat16
SCORE = float(np.log2(np.e) / np.sqrt(HD))

SLOTS = ((0, 0), (0, 2), (0, 3), (1, 2), (0, 1), (1, 3), (1, 1), (1, 0))
DX_BITS = sum(dx << j for j, (dx, _) in enumerate(SLOTS))
DY_BITS = sum(dy << (2 * j) for j, (_, dy) in enumerate(SLOTS))

UP, DOWN, ACROSS, BEYOND, ZUP, ZDOWN, CORE = range(7)
OWN, FAR, NEAR_M, NEAR_P = range(4)
R_HALF, R_P, R_M = range(3)

QUARTERS = [(q * CH, CH) for q in range(NQ)]
HALF = ROWS_B // 2
HALVES = [(0, HALF), (HALF, HALF)]
EIGHTHS = [(q * CH, CH, r * HALF, HALF) for r in range(2) for q in range(NQ)]
ROUTES = {
    "own_up": (UP, "x", 0, "x", 2, QUARTERS),
    "own_down": (DOWN, "x", 0, "x", 4, QUARTERS),
    "own_across": (ACROSS, "x", 0, "x", 7, QUARTERS),
    "far_up": (UP, "x", 2, "x", 1, QUARTERS[:2]),
    "far_down": (DOWN, "x", 4, "x", 1, QUARTERS[2:]),
    "far_across": (ACROSS, "x", 1, "x", 3, QUARTERS),
    "side_up": (UP, "x", 7, "x", 5, QUARTERS),
    "side_down": (DOWN, "x", 7, "x", 6, QUARTERS),
    "att_own": (ACROSS, "a", 7, "b", OWN, HALVES),
    "att_far": (ACROSS, "a", 3, "b", FAR, HALVES),
    "att_near_m": (ACROSS, "a", 5, "b", NEAR_M, HALVES),
    "att_near_p": (ACROSS, "a", 6, "b", NEAR_P, HALVES),
    "half_down": (DOWN, "p", FAR, "r", R_HALF, QUARTERS[:2]),
    "half_up": (UP, "p", FAR, "r", R_HALF, QUARTERS[2:]),
    "sum_down": (DOWN, "p", NEAR_M, "r", R_P, EIGHTHS),
    "sum_up": (UP, "p", NEAR_P, "r", R_M, EIGHTHS),
}
WEIGHTS = {
    "w_beyond": (BEYOND, True, 0, (0, 1, 2, 3)),
    "w_zup": (ZUP, False, 0, (0, 1, 2, 3)),
    "w_zdown": (ZDOWN, False, 0, (0, 1, 2, 3)),
    "w_fwd_up": (ZUP, False, 3, (0, 1)),
    "w_fwd_down": (ZDOWN, False, 1, (2, 3)),
    "w_core0": (CORE, False, 0, (None,)),
    "w_core3": (CORE, False, 3, (None,)),
    "w_core1": (CORE, False, 1, (None,)),
    "w_core2": (CORE, False, 2, (None,)),
}
BASE = {}
COUNT = 0
for _name, _spec in ROUTES.items():
    BASE[_name] = COUNT
    COUNT += len(_spec[5])
for _name, _spec in WEIGHTS.items():
    BASE[_name] = COUNT
    COUNT += len(_spec[3])
PIECE = QC // 8
SUB = PIECE // 4


def body(
    tokens_hbm, gain_hbm, wq_hbm, wk_hbm, wv_hbm, wo_hbm, kv_hbm, exps_hbm, cos_hbm, sin_hbm,
    pad_hbm, unpad_hbm, pad_k_hbm, pad_v_hbm, parity_hbm, raw,
    xg, pb, rb, ab, bb, w_in, w_out, w_two, kv, acc, qkv, qp, kp, vp, ap, exps, gains,
    gain_ref, exps_ref, cos_ref, sin_ref, pad_ref, unpad_ref, pad_k_ref, pad_v_ref, parity_ref,
    load_sem, send_sem, recv_sem,
):
    me = lax.axis_index("tensor")
    mx, my = me // 4, me % 4
    dp = lax.axis_index("dp")
    hi, z, core = dp // 8, (dp // 2) % 4, dp % 2
    other = (1 - mx) * 4 + my
    z_next, z_last = (z + 1) % 4, (z + 3) % 4
    targets = {
        UP: {"tensor": mx * 4 + (my + 1) % 4},
        DOWN: {"tensor": mx * 4 + (my + 3) % 4},
        ACROSS: {"tensor": other},
        BEYOND: {"dp": (1 - hi) * 8 + z * 2 + core, "tensor": other},
        ZUP: {"dp": hi * 8 + z_next * 2 + core},
        ZDOWN: {"dp": hi * 8 + z_last * 2 + core},
        CORE: {"dp": hi * 8 + z * 2 + (1 - core)},
    }
    buffers = {"x": xg, "p": pb, "r": rb, "a": ab, "b": bb}

    def route(name, i):
        k = BASE[name] + i
        if name in ROUTES:
            target, sbuf, sslot, dbuf, dslot, pieces = ROUTES[name]
            at = pl.ds(*pieces[i][:2])
            if len(pieces[i]) == 4:
                rows = pl.ds(*pieces[i][2:])
                src, dst = buffers[sbuf].at[sslot, rows, at], buffers[dbuf].at[dslot, rows, at]
            elif sbuf == "a":
                src, dst = ab.at[sslot, at, :], bb.at[dslot, at, :]
            else:
                src, dst = buffers[sbuf].at[sslot, :, at], buffers[dbuf].at[dslot, :, at]
        else:
            target, mine, dz, subs = WEIGHTS[name]
            first = (((z + dz) % 4) * 2 + core) * PIECE
            if subs[i] is None:
                rows = pl.ds(pl.multiple_of(first, PIECE), PIECE)
            else:
                rows = pl.ds(pl.multiple_of(first + subs[i] * SUB, SUB), SUB)
            src, dst = (w_out if mine else w_two).at[rows, :], w_two.at[rows, :]
        return pltpu.make_async_remote_copy(
            src_ref=src, dst_ref=dst, send_sem=send_sem.at[k], recv_sem=recv_sem.at[k],
            device_id=targets[target], device_id_type=MESH,
        )

    def pieces_of(name, which):
        if which is not None:
            return which
        return range(len(ROUTES[name][5] if name in ROUTES else WEIGHTS[name][3]))

    def send(name, which=None):
        for i in pieces_of(name, which):
            route(name, i).start()

    def arrived(name, which=None):
        for i in pieces_of(name, which):
            received(name, i).wait_recv()

    def received(name, i):
        if name in ROUTES:
            return route(name, i)
        k = BASE[name] + i
        target, _, dz, subs = WEIGHTS[name]
        sender_z = {BEYOND: z, ZUP: z_last, ZDOWN: z_next, CORE: z}[target]
        sender_core = (1 - core) if target == CORE else core
        first = (((sender_z + dz) % 4) * 2 + sender_core) * PIECE
        if subs[i] is None:
            rows = pl.ds(pl.multiple_of(first, PIECE), PIECE)
        else:
            rows = pl.ds(pl.multiple_of(first + subs[i] * SUB, SUB), SUB)
        return pltpu.make_async_remote_copy(
            src_ref=w_two.at[rows, :], dst_ref=w_two.at[rows, :], send_sem=send_sem.at[k],
            recv_sem=recv_sem.at[k], device_id=targets[target], device_id_type=MESH,
        )

    def norm():
        def some(i5, c):
            squares = []
            for i in range(5):
                rows = pl.ds(pl.multiple_of((i5 * 5 + i) * 16, 16), 16)
                total = None
                for g in range(D // HD):
                    x = raw[rows, g * HD : (g + 1) * HD].astype(F32)
                    total = x * x if g == 0 else total + x * x
                squares.append(total)
            scales = [
                lax.rsqrt(jnp.sum(x, axis=-1, keepdims=True) * (1.0 / D) + EPS) for x in squares
            ]
            for i in range(5):
                rows = pl.ds(pl.multiple_of((i5 * 5 + i) * 16, 16), 16)
                xg[0, rows, :] = (raw[rows, :].astype(F32) * scales[i] * gains[...]).astype(BF16)
            return c

        lax.fori_loop(0, 2, some, 0)

    barrier = pltpu.get_barrier_semaphore()
    for target in targets.values():
        pl.semaphore_signal(barrier, inc=1, device_id=target, device_id_type=MESH)
    load_x = pltpu.make_async_copy(tokens_hbm, raw, load_sem.at[0])
    load_o = pltpu.make_async_copy(wo_hbm, w_out, load_sem.at[1])
    load_q = pltpu.make_async_copy(wq_hbm, w_in.at[:, pl.ds(0, QC)], load_sem.at[2])
    load_k = pltpu.make_async_copy(wk_hbm, w_in.at[:, pl.ds(QC, HD)], load_sem.at[3])
    load_v = pltpu.make_async_copy(wv_hbm, w_in.at[:, pl.ds(QC + HD, HD)], load_sem.at[4])
    load_kv = pltpu.make_async_copy(kv_hbm, kv, load_sem.at[5])
    small = [
        pltpu.make_async_copy(src, dst, load_sem.at[6 + i])
        for i, (src, dst) in enumerate((
            (gain_hbm, gain_ref), (exps_hbm, exps_ref), (cos_hbm, cos_ref), (sin_hbm, sin_ref),
            (pad_hbm, pad_ref), (unpad_hbm, unpad_ref), (pad_k_hbm, pad_k_ref),
            (pad_v_hbm, pad_v_ref), (parity_hbm, parity_ref),
        ))
    ]
    for copy in (small[0], load_x, load_o, *small[1:], load_q, load_k, load_v, load_kv):
        copy.start()
    small[0].wait()
    gain = gain_ref[...].astype(F32)
    for g in range(D // HD):
        gains[:, g * HD : (g + 1) * HD] = jnp.broadcast_to(gain[g : g + 1], (16, HD))
    load_x.wait()
    norm()
    pl.semaphore_wait(barrier, len(targets))

    for i in range(NQ):
        if i < 2:
            send("own_up", (i,))
            send("own_down", (i + 2,))
        if i < 3:
            send("own_across", (i,))
    load_o.wait()
    send("w_beyond")

    for copy in small[1:]:
        copy.wait()
    fill = jnp.zeros((HD - 32, HD), F32)
    for i in range(8 * ROWS_B // HD):
        at = slice(i * HD, (i + 1) * HD)
        exps[at, :] = jnp.concatenate([exps_ref[:, at].astype(F32), fill], 0).T

    def rot(m):
        return m * cos_ref[...] + pltpu.roll(m, HD // 2, 1) * sin_ref[...]

    def turn(m, n):
        second_head = rot(m[:, HD:]) if n < 4 else m[:, HD:]
        return jnp.concatenate([rot(m[:, :HD]), second_head], 1).astype(BF16)

    def project(j):
        for n in range(5):
            at = slice(n * 256, (n + 1) * 256)
            m = jnp.dot(xg[j], w_in[:, at], preferred_element_type=F32)
            qkv[0, :, at] = turn(m, n)

    early = 3 * CH

    def project_sides(first):
        for n in range(5):
            at = slice(n * 256, (n + 1) * 256)
            if first:
                rows = xg[5:7, :, :early].reshape(2 * ROWS_B, early)
                acc[:, at] = jnp.dot(rows, w_in[:early, at], preferred_element_type=F32)
            else:
                rows = xg[5:7, :, early:].reshape(2 * ROWS_B, D - early)
                m = acc[:, at] + jnp.dot(rows, w_in[early:, at], preferred_element_type=F32)
                for i in range(2):
                    qkv[i, :, at] = turn(m[i * ROWS_B : (i + 1) * ROWS_B], n)

    def spread_out(i):
        for n in range(4):
            at = slice(n * 256, (n + 1) * 256)
            qp[:, at] = jnp.dot(
                pad_ref[...], qkv[i, :, at], preferred_element_type=F32
            ).astype(BF16)
        kp[...] = jnp.dot(
            pad_k_ref[...], qkv[i, :, QC : QC + HD], preferred_element_type=F32
        ).astype(BF16)
        vp[...] = jnp.dot(
            pad_v_ref[...], qkv[i, :, QC + HD :], preferred_element_type=F32
        ).astype(BF16)

    def attend(j, t, half):
        lane = lax.broadcasted_iota(jnp.int32, (HD, HD), 1)
        token = lax.broadcasted_iota(jnp.int32, (HD, HD), 0) % 16
        seen = (lane % 2 == 0) | (lane <= 2 * token + 1)
        contract_last = (((1,), (1,)), ((), ()))
        batch = 4

        def some(s4, c):
            scores, values = [], []
            for i in range(batch):
                s = s4 * batch + i
                rows = pl.ds(pl.multiple_of(s * 16, 16), 16)
                spread = pl.ds(pl.multiple_of(s * 32, 32), 32)
                query = jnp.concatenate([qp[rows, h * HD : (h + 1) * HD] for h in range(HEADS)], 0)
                pairs = kv[t * SEQ_BLOCK + s]
                keys = jnp.concatenate([pairs[:32] * parity_ref[0] + kp[spread, :], pairs[32:]], 0)
                values.append(
                    jnp.concatenate([pairs[:32] * parity_ref[1] + vp[spread, :], pairs[32:]], 0)
                )
                scores.append(
                    lax.dot_general(query, keys, contract_last, preferred_element_type=F32)
                )
            scores = [jnp.where(seen, x, -1e30) for x in scores]
            tops = [jnp.max(x, axis=1, keepdims=True) for x in scores]
            raised = [jnp.exp2((x - top) * SCORE) for x, top in zip(scores, tops)]
            totals = [jnp.sum(x, axis=1, keepdims=True) for x in raised]
            probs = [(x * (1.0 / total)).astype(BF16) for x, total in zip(raised, totals)]
            for i in range(batch):
                rows = pl.ds(pl.multiple_of((s4 * batch + i) * 16, 16), 16)
                p = pltpu.roll(probs[i], 1, 1)
                att = jnp.dot(p, values[i], preferred_element_type=F32).astype(BF16)
                for h in range(HEADS):
                    ap[rows, h * HD : (h + 1) * HD] = att[h * 16 : (h + 1) * 16]
            return c

        parts = SEQ_BLOCK // batch // 2
        lax.fori_loop(half * parts, (half + 1) * parts, some, 0)
        rows = slice(half * 80, (half + 1) * 80)
        for n in range(4):
            at = slice(n * 256, (n + 1) * 256)
            padded = ap[half * 128 : (half + 1) * 128, at]
            ab[j, rows, at] = jnp.dot(
                unpad_ref[...], padded, preferred_element_type=F32
            ).astype(BF16)

    def powers(t, sign, first=0, count=ROWS_B):
        e = exps[pl.ds(pl.multiple_of(t * ROWS_B + first, 16), count), :].astype(jnp.int32)
        if sign < 0:
            return jnp.left_shift(1, -e).astype(F32)
        return jnp.left_shift(1, e + 11).astype(F32) * (2.0**-11)

    def out_project(att, weights, k, t, order, extra, done, first=0, count=ROWS_B):
        shrink = powers(t, -1, first, count)
        rows = slice(first, first + count)
        for q in order:
            for base in (q * CH, q * CH + 512):
                part = jnp.dot(att, weights[:, base : base + 512], preferred_element_type=F32)
                for g in range(4):
                    at = slice(base + g * HD, base + (g + 1) * HD)
                    group = base // HD + g
                    scaled = part[:, g * HD : (g + 1) * HD] * shrink[:, group : group + 1]
                    scaled = jnp.clip(scaled, -127.0, 127.0).astype(BF16)
                    for r in extra(q, g == 0 and base == q * CH):
                        scaled = scaled.astype(F32) + r[rows, at].astype(F32)
                    pb[k, rows, at] = scaled.astype(BF16)
            done(q)

    def column_block(j):
        return j - j // 4

    def second(k, dy, order, send_sum, half=None, part=None):
        first, count = HALVES[part] if part is not None else (0, ROWS_B)

        def extra(q, opening):
            refs = [pb.at[k]]
            if half is not None and q in half[1]:
                if opening and part == 0:
                    arrived(half[0], (half[1].index(q),))
                refs.append(rb.at[R_HALF])
            return refs

        out_project(
            bb[k, first : first + count], w_two, k, mx * 4 + (my + dy) % 4, order, extra, send_sum,
            first, count,
        )

    def near(up, part, order):
        name = "sum_up" if up else "sum_down"

        def send_sum(q):
            send(name, (part * NQ + q,))

        if up:
            second(NEAR_P, 1, order, send_sum, ("half_up", (2, 3)), part)
        else:
            second(NEAR_M, 3, order, send_sum, ("half_down", (0, 1)), part)

    def when(j, k, action):
        pl.when(j == k)(action)

    def before(j):
        @functools.partial(when, j, 1)
        def _():
            arrived("own_up", (0,))
            send("far_up", (0,))
            send("own_up", (2,))
            arrived("own_down", (2,))
            send("far_down", (0,))
            send("own_down", (0,))
            for i in range(4):
                arrived("w_beyond", (i,))
                send("w_zup", (i,))
                send("w_zdown", (i,))
                if i == 1:
                    arrived("own_up", (1,))
                    send("far_up", (1,))
                    send("own_up", (3,))
                    arrived("own_down", (3,))
                    send("far_down", (1,))
                    send("own_down", (1,))
            arrived("far_up", (0,))
            send("far_across", (0,))
            arrived("far_down", (0,))
            send("far_across", (2,))
            send("w_core0")
            arrived("own_across", (0, 1, 2))
            send("side_up", (0, 1, 2))
            send("side_down", (0, 1, 2))
            arrived("w_zup", (0, 1))
            send("w_fwd_up")
            arrived("w_zdown", (2, 3))
            send("w_fwd_down")
            arrived("far_up", (1,))
            send("far_across", (1,))
            arrived("far_down", (1,))
            send("far_across", (3,))
            send("own_across", (3,))

        @functools.partial(when, j, 2)
        def _():
            arrived("w_zup", (2, 3))
            send("w_core3")
            arrived("w_zdown", (0, 1))
            send("w_core1")
            arrived("own_up", (2, 3))

        @functools.partial(when, j, 3)
        def _():
            arrived("w_fwd_up")
            arrived("w_fwd_down")
            send("w_core2")
            arrived("far_across")

        @functools.partial(when, j, 4)
        def _():
            arrived("own_down", (0, 1))
            arrived("own_across", (3,))
            send("side_up", (3,))
            send("side_down", (3,))

        @functools.partial(when, j, 5)
        def _():
            for name in ("w_core0", "w_core3", "w_core1", "w_core2"):
                arrived(name)
            arrived("att_far")
            second(FAR, 2, (0, 2, 1, 3), lambda q: send("half_down" if q < 2 else "half_up", (q % 2,)))
            arrived("side_up", (0, 1, 2))
            arrived("side_down", (0, 1, 2))
            project_sides(True)
            arrived("side_up", (3,))
            arrived("side_down", (3,))
            project_sides(False)

        @functools.partial(when, j, 7)
        def _():
            arrived("att_near_m", (0,))
            near(False, 0, (2, 3))
            arrived("att_near_p", (0,))
            near(True, 0, (0, 1))
            near(False, 0, (0, 1))
            near(True, 0, (2, 3))
            arrived("att_near_m", (1,))
            near(False, 1, (2, 3, 0, 1))
            arrived("att_near_p", (1,))
            near(True, 1, (0, 1, 2, 3))

    def step(j, c):
        dx = (DX_BITS >> j) & 1
        dy = (DY_BITS >> (2 * j)) & 3
        t = ((mx + dx) % 2) * 4 + (my + dy) % 4
        before(j)

        @pl.when((j < 5) | (j == 7))
        def _():
            project(j)

        spread_out(j // 6 - j // 7)
        for half in range(2):
            attend(j, t, half)
            when(j, 3, functools.partial(send, "att_far", (half,)))
            when(j, 7, functools.partial(send, "att_own", (half,)))
            if half == 0:
                when(j, 5, functools.partial(send, "att_near_m", (0,)))
            when(j, 6, functools.partial(send, "att_near_p", (half,)))
            if half == 0:
                when(j, 6, functools.partial(send, "att_near_m", (1,)))

        @pl.when(dx == 0)
        def _():
            out_project(
                ab[j], w_out, column_block(j), t, range(NQ), lambda q, first: (), lambda q: None
            )

        return c

    load_q.wait()
    load_k.wait()
    load_v.wait()
    load_kv.wait()
    lax.fori_loop(0, 8, step, 0)

    arrived("att_own")
    second(OWN, 0, range(NQ), lambda q: None)

    restore = powers(me, 1)
    for part in range(2):
        rows = slice(part * HALF, (part + 1) * HALF)
        for q in (0, 2, 1, 3):
            arrived("sum_down", (part * NQ + q,))
            arrived("sum_up", (part * NQ + q,))
            for g in range(CH // HD):
                group = q * (CH // HD) + g
                at = slice(group * HD, (group + 1) * HD)
                total = pb[OWN, rows, at].astype(F32)
                for r in (R_P, R_M):
                    total = total + rb[r, rows, at].astype(F32)
                mixed = raw[rows, at].astype(F32) + total * restore[rows, group : group + 1]
                raw[rows, at] = mixed.astype(BF16)
    for name in (*ROUTES, *WEIGHTS):
        for i in pieces_of(name, None):
            route(name, i).wait_send()


def tables():
    position = (np.arange(ROWS_B) % NEW + CACHE).astype(np.float32)
    frequency = THETA ** (-(np.arange(HD // 2, dtype=np.float32) * np.float32(2.0)) / np.float32(HD))
    angles = position[:, None] * frequency.astype(np.float32)[None, :]
    cosine, sine = np.cos(angles), np.sin(angles)
    row = np.arange(ROWS_B)
    spread = np.zeros((PADDED, ROWS_B), np.float32)
    spread[row // NEW * 16 + row % NEW, row] = 1.0
    keys = np.zeros((SPREAD, ROWS_B), np.float32)
    keys[row // NEW * 32 + 2 * (row % NEW) + 1, row] = 1.0
    values = np.zeros((SPREAD, ROWS_B), np.float32)
    values[row // NEW * 32 + 2 * (row % NEW) + 2, row] = 1.0
    even = np.broadcast_to((np.arange(32) % 2 == 0)[:, None], (32, HD))
    return (
        jnp.asarray(np.concatenate([cosine, cosine], 1), F32),
        jnp.asarray(np.concatenate([-sine, sine], 1), F32),
        jnp.asarray(spread, BF16),
        jnp.asarray(spread.T[: ROWS_B // 2, : PADDED // 2], BF16),
        jnp.asarray(keys, BF16),
        jnp.asarray(values, BF16),
        jnp.asarray(np.stack([even, ~even]), BF16),
    )


def on_device(
    tokens, norm_gain, query_weight, key_weight, value_weight, out_weight, past_cache, exponents
):
    seqs = past_cache.shape[0]
    pairs = past_cache.reshape(seqs, 2 * CACHE, HD)
    anywhere = pl.BlockSpec(memory_space=pl.ANY)
    return pl.pallas_call(
        body,
        out_shape=pltpu.VMEM(tokens.shape, BF16),
        in_specs=[anywhere] * 15,
        out_specs=pl.BlockSpec(memory_space=pltpu.VMEM),
        scratch_shapes=[
            pltpu.VMEM((8, ROWS_B, D), BF16),
            pltpu.VMEM((4, ROWS_B, D), BF16),
            pltpu.VMEM((3, ROWS_B, D), BF16),
            pltpu.VMEM((8, ROWS_B, QC), BF16),
            pltpu.VMEM((4, ROWS_B, QC), BF16),
            pltpu.VMEM((D, QC + 2 * HD), BF16),
            pltpu.VMEM((QC, D), BF16),
            pltpu.VMEM((QC, D), BF16),
            pltpu.VMEM((seqs, 2 * CACHE, HD), BF16),
            pltpu.VMEM((2 * ROWS_B, QC + 2 * HD), F32),
            pltpu.VMEM((2, ROWS_B, QC + 2 * HD), BF16),
            pltpu.VMEM((PADDED, QC), BF16),
            pltpu.VMEM((SPREAD, HD), BF16),
            pltpu.VMEM((SPREAD, HD), BF16),
            pltpu.VMEM((PADDED, QC), BF16),
            pltpu.VMEM((8 * ROWS_B, HD), F32),
            pltpu.VMEM((16, D), F32),
            pltpu.VMEM((D // HD, HD), BF16),
            pltpu.VMEM((D // HD, exponents.shape[0]), jnp.int32),
            pltpu.VMEM((ROWS_B, HD), F32),
            pltpu.VMEM((ROWS_B, HD), F32),
            pltpu.VMEM((PADDED, ROWS_B), BF16),
            pltpu.VMEM((ROWS_B // 2, PADDED // 2), BF16),
            pltpu.VMEM((SPREAD, ROWS_B), BF16),
            pltpu.VMEM((SPREAD, ROWS_B), BF16),
            pltpu.VMEM((2, 32, HD), BF16),
            pltpu.SemaphoreType.DMA((15,)),
            pltpu.SemaphoreType.DMA((COUNT,)),
            pltpu.SemaphoreType.DMA((COUNT,)),
        ],
        compiler_params=pltpu.CompilerParams(
            collective_id=0, has_side_effects=True, vmem_limit_bytes=64_000_000
        ),
        name="verify_block",
    )(
        tokens, norm_gain.reshape(D // HD, HD), query_weight, key_weight, value_weight, out_weight,
        pairs, exponents.T, *tables(),
    )


def solution(mesh):
    return jax.shard_map(
        on_device,
        mesh=mesh,
        in_specs=(
            P(("dp", "tensor"), None),
            P(),
            P(None, "tensor"),
            P(None, "tensor"),
            P(None, "tensor"),
            P("tensor", None),
            P("dp", None, None, "tensor"),
            P("dp", None),
        ),
        out_specs=P(("dp", "tensor"), None),
        check_vma=False,
    )
```

```python
import functools

import jax
import jax.numpy as jnp
import numpy as np
from jax import lax
from jax.experimental import pallas as pl
from jax.experimental.pallas import tpu as pltpu
from jax.sharding import PartitionSpec as P

HD = 128
NEW = 10
CACHE = 64
D = 4096
HEADS = 8
QC = 1024
SEQ_BLOCK = 16
ROWS_B = 160
PADDED = 256
SPREAD = 512
CH = 1024
NQ = 4
EPS = 1e-05
THETA = 500000.0
MESH = pl.DeviceIdType.MESH
F32 = jnp.float32
BF16 = jnp.bfloat16
SCORE = float(np.log2(np.e) / np.sqrt(HD))

SLOTS = ((0, 0), (0, 2), (0, 3), (1, 2), (0, 1), (1, 3), (1, 1), (1, 0))
DX_BITS = sum(dx << j for j, (dx, _) in enumerate(SLOTS))
DY_BITS = sum(dy << (2 * j) for j, (_, dy) in enumerate(SLOTS))

UP, DOWN, ACROSS, BEYOND, ZUP, ZDOWN, CORE = range(7)
OWN, FAR, NEAR_M, NEAR_P = range(4)
R_HALF, R_P, R_M = range(3)

QUARTERS = [(q * CH, CH) for q in range(NQ)]
HALF = ROWS_B // 2
HALVES = [(0, HALF), (HALF, HALF)]
EIGHTHS = [(q * CH, CH, r * HALF, HALF) for r in range(2) for q in range(NQ)]
ROUTES = {
    "own_up": (UP, "x", 0, "x", 2, QUARTERS),
    "own_down": (DOWN, "x", 0, "x", 4, QUARTERS),
    "own_across": (ACROSS, "x", 0, "x", 7, QUARTERS),
    "far_up": (UP, "x", 2, "x", 1, QUARTERS[:2]),
    "far_down": (DOWN, "x", 4, "x", 1, QUARTERS[2:]),
    "far_across": (ACROSS, "x", 1, "x", 3, QUARTERS),
    "side_up": (UP, "x", 7, "x", 5, QUARTERS),
    "side_down": (DOWN, "x", 7, "x", 6, QUARTERS),
    "att_own": (ACROSS, "a", 7, "b", OWN, HALVES),
    "att_far": (ACROSS, "a", 3, "b", FAR, HALVES),
    "att_near_m": (ACROSS, "a", 5, "b", NEAR_M, HALVES),
    "att_near_p": (ACROSS, "a", 6, "b", NEAR_P, HALVES),
    "half_down": (DOWN, "p", FAR, "r", R_HALF, QUARTERS[:2]),
    "half_up": (UP, "p", FAR, "r", R_HALF, QUARTERS[2:]),
    "sum_down": (DOWN, "p", NEAR_M, "r", R_P, EIGHTHS),
    "sum_up": (UP, "p", NEAR_P, "r", R_M, EIGHTHS),
}
WEIGHTS = {
    "w_beyond": (BEYOND, True, 0, (0, 1, 2, 3)),
    "w_zup": (ZUP, False, 0, (0, 1, 2, 3)),
    "w_zdown": (ZDOWN, False, 0, (0, 1, 2, 3)),
    "w_fwd_up": (ZUP, False, 3, (0, 1)),
    "w_fwd_down": (ZDOWN, False, 1, (2, 3)),
    "w_core0": (CORE, False, 0, (None,)),
    "w_core3": (CORE, False, 3, (None,)),
    "w_core1": (CORE, False, 1, (None,)),
    "w_core2": (CORE, False, 2, (None,)),
}
BASE = {}
COUNT = 0
for _name, _spec in ROUTES.items():
    BASE[_name] = COUNT
    COUNT += len(_spec[5])
for _name, _spec in WEIGHTS.items():
    BASE[_name] = COUNT
    COUNT += len(_spec[3])
PIECE = QC // 8
SUB = PIECE // 4


def body(
    tokens_hbm, gain_hbm, wq_hbm, wk_hbm, wv_hbm, wo_hbm, kv_hbm, exps_hbm, cos_hbm, sin_hbm,
    pad_hbm, unpad_hbm, pad_k_hbm, pad_v_hbm, parity_hbm, raw,
    xg, pb, rb, ab, bb, w_in, w_out, w_two, kv, acc, qkv, qp, kp, vp, ap, exps, gains,
    gain_ref, exps_ref, cos_ref, sin_ref, pad_ref, unpad_ref, pad_k_ref, pad_v_ref, parity_ref,
    load_sem, send_sem, recv_sem,
):
    me = lax.axis_index("tensor")
    mx, my = me // 4, me % 4
    dp = lax.axis_index("dp")
    hi, z, core = dp // 8, (dp // 2) % 4, dp % 2
    other = (1 - mx) * 4 + my
    z_next, z_last = (z + 1) % 4, (z + 3) % 4
    targets = {
        UP: {"tensor": mx * 4 + (my + 1) % 4},
        DOWN: {"tensor": mx * 4 + (my + 3) % 4},
        ACROSS: {"tensor": other},
        BEYOND: {"dp": (1 - hi) * 8 + z * 2 + core, "tensor": other},
        ZUP: {"dp": hi * 8 + z_next * 2 + core},
        ZDOWN: {"dp": hi * 8 + z_last * 2 + core},
        CORE: {"dp": hi * 8 + z * 2 + (1 - core)},
    }
    buffers = {"x": xg, "p": pb, "r": rb, "a": ab, "b": bb}

    def route(name, i):
        k = BASE[name] + i
        if name in ROUTES:
            target, sbuf, sslot, dbuf, dslot, pieces = ROUTES[name]
            at = pl.ds(*pieces[i][:2])
            if len(pieces[i]) == 4:
                rows = pl.ds(*pieces[i][2:])
                src, dst = buffers[sbuf].at[sslot, rows, at], buffers[dbuf].at[dslot, rows, at]
            elif sbuf == "a":
                src, dst = ab.at[sslot, at, :], bb.at[dslot, at, :]
            else:
                src, dst = buffers[sbuf].at[sslot, :, at], buffers[dbuf].at[dslot, :, at]
        else:
            target, mine, dz, subs = WEIGHTS[name]
            first = (((z + dz) % 4) * 2 + core) * PIECE
            if subs[i] is None:
                rows = pl.ds(pl.multiple_of(first, PIECE), PIECE)
            else:
                rows = pl.ds(pl.multiple_of(first + subs[i] * SUB, SUB), SUB)
            src, dst = (w_out if mine else w_two).at[rows, :], w_two.at[rows, :]
        return pltpu.make_async_remote_copy(
            src_ref=src, dst_ref=dst, send_sem=send_sem.at[k], recv_sem=recv_sem.at[k],
            device_id=targets[target], device_id_type=MESH,
        )

    def pieces_of(name, which):
        if which is not None:
            return which
        return range(len(ROUTES[name][5] if name in ROUTES else WEIGHTS[name][3]))

    def send(name, which=None):
        for i in pieces_of(name, which):
            route(name, i).start()

    def arrived(name, which=None):
        for i in pieces_of(name, which):
            received(name, i).wait_recv()

    def received(name, i):
        if name in ROUTES:
            return route(name, i)
        k = BASE[name] + i
        target, _, dz, subs = WEIGHTS[name]
        sender_z = {BEYOND: z, ZUP: z_last, ZDOWN: z_next, CORE: z}[target]
        sender_core = (1 - core) if target == CORE else core
        first = (((sender_z + dz) % 4) * 2 + sender_core) * PIECE
        if subs[i] is None:
            rows = pl.ds(pl.multiple_of(first, PIECE), PIECE)
        else:
            rows = pl.ds(pl.multiple_of(first + subs[i] * SUB, SUB), SUB)
        return pltpu.make_async_remote_copy(
            src_ref=w_two.at[rows, :], dst_ref=w_two.at[rows, :], send_sem=send_sem.at[k],
            recv_sem=recv_sem.at[k], device_id=targets[target], device_id_type=MESH,
        )

    def norm():
        def some(i5, c):
            squares = []
            for i in range(5):
                rows = pl.ds(pl.multiple_of((i5 * 5 + i) * 16, 16), 16)
                total = None
                for g in range(D // HD):
                    x = raw[rows, g * HD : (g + 1) * HD].astype(F32)
                    total = x * x if g == 0 else total + x * x
                squares.append(total)
            scales = [
                lax.rsqrt(jnp.sum(x, axis=-1, keepdims=True) * (1.0 / D) + EPS) for x in squares
            ]
            for i in range(5):
                rows = pl.ds(pl.multiple_of((i5 * 5 + i) * 16, 16), 16)
                xg[0, rows, :] = (raw[rows, :].astype(F32) * scales[i] * gains[...]).astype(BF16)
            return c

        lax.fori_loop(0, 2, some, 0)

    barrier = pltpu.get_barrier_semaphore()
    for target in targets.values():
        pl.semaphore_signal(barrier, inc=1, device_id=target, device_id_type=MESH)
    load_x = pltpu.make_async_copy(tokens_hbm, raw, load_sem.at[0])
    load_o = pltpu.make_async_copy(wo_hbm, w_out, load_sem.at[1])
    load_q = pltpu.make_async_copy(wq_hbm, w_in.at[:, pl.ds(0, QC)], load_sem.at[2])
    load_k = pltpu.make_async_copy(wk_hbm, w_in.at[:, pl.ds(QC, HD)], load_sem.at[3])
    load_v = pltpu.make_async_copy(wv_hbm, w_in.at[:, pl.ds(QC + HD, HD)], load_sem.at[4])
    load_kv = pltpu.make_async_copy(kv_hbm, kv, load_sem.at[5])
    small = [
        pltpu.make_async_copy(src, dst, load_sem.at[6 + i])
        for i, (src, dst) in enumerate((
            (gain_hbm, gain_ref), (exps_hbm, exps_ref), (cos_hbm, cos_ref), (sin_hbm, sin_ref),
            (pad_hbm, pad_ref), (unpad_hbm, unpad_ref), (pad_k_hbm, pad_k_ref),
            (pad_v_hbm, pad_v_ref), (parity_hbm, parity_ref),
        ))
    ]
    for copy in (small[0], load_x, load_o, *small[1:], load_q, load_k, load_v, load_kv):
        copy.start()
    small[0].wait()
    gain = gain_ref[...].astype(F32)
    for g in range(D // HD):
        gains[:, g * HD : (g + 1) * HD] = jnp.broadcast_to(gain[g : g + 1], (16, HD))
    load_x.wait()
    norm()
    pl.semaphore_wait(barrier, len(targets))

    for i in range(NQ):
        if i < 2:
            send("own_up", (i,))
            send("own_down", (i + 2,))
        if i < 3:
            send("own_across", (i,))
    load_o.wait()
    send("w_beyond")

    for copy in small[1:]:
        copy.wait()
    fill = jnp.zeros((HD - 32, HD), F32)
    for i in range(8 * ROWS_B // HD):
        at = slice(i * HD, (i + 1) * HD)
        exps[at, :] = jnp.concatenate([exps_ref[:, at].astype(F32), fill], 0).T

    def rot(m):
        return m * cos_ref[...] + pltpu.roll(m, HD // 2, 1) * sin_ref[...]

    def turn(m, n):
        second_head = rot(m[:, HD:]) if n < 4 else m[:, HD:]
        return jnp.concatenate([rot(m[:, :HD]), second_head], 1).astype(BF16)

    def project(j):
        for n in range(5):
            at = slice(n * 256, (n + 1) * 256)
            m = jnp.dot(xg[j], w_in[:, at], preferred_element_type=F32)
            qkv[0, :, at] = turn(m, n)

    early = 3 * CH

    def project_sides(first):
        for n in range(5):
            at = slice(n * 256, (n + 1) * 256)
            if first:
                rows = xg[5:7, :, :early].reshape(2 * ROWS_B, early)
                acc[:, at] = jnp.dot(rows, w_in[:early, at], preferred_element_type=F32)
            else:
                rows = xg[5:7, :, early:].reshape(2 * ROWS_B, D - early)
                m = acc[:, at] + jnp.dot(rows, w_in[early:, at], preferred_element_type=F32)
                for i in range(2):
                    qkv[i, :, at] = turn(m[i * ROWS_B : (i + 1) * ROWS_B], n)

    def spread_out(i):
        for n in range(4):
            at = slice(n * 256, (n + 1) * 256)
            qp[:, at] = jnp.dot(
                pad_ref[...], qkv[i, :, at], preferred_element_type=F32
            ).astype(BF16)
        kp[...] = jnp.dot(
            pad_k_ref[...], qkv[i, :, QC : QC + HD], preferred_element_type=F32
        ).astype(BF16)
        vp[...] = jnp.dot(
            pad_v_ref[...], qkv[i, :, QC + HD :], preferred_element_type=F32
        ).astype(BF16)

    def attend(j, t, half):
        lane = lax.broadcasted_iota(jnp.int32, (HD, HD), 1)
        token = lax.broadcasted_iota(jnp.int32, (HD, HD), 0) % 16
        seen = (lane % 2 == 0) | (lane <= 2 * token + 1)
        contract_last = (((1,), (1,)), ((), ()))
        batch = 4

        def some(s4, c):
            scores, values = [], []
            for i in range(batch):
                s = s4 * batch + i
                rows = pl.ds(pl.multiple_of(s * 16, 16), 16)
                spread = pl.ds(pl.multiple_of(s * 32, 32), 32)
                query = jnp.concatenate([qp[rows, h * HD : (h + 1) * HD] for h in range(HEADS)], 0)
                pairs = kv[t * SEQ_BLOCK + s]
                keys = jnp.concatenate([pairs[:32] * parity_ref[0] + kp[spread, :], pairs[32:]], 0)
                values.append(
                    jnp.concatenate([pairs[:32] * parity_ref[1] + vp[spread, :], pairs[32:]], 0)
                )
                scores.append(
                    lax.dot_general(query, keys, contract_last, preferred_element_type=F32)
                )
            scores = [jnp.where(seen, x, -1e30) for x in scores]
            tops = [jnp.max(x, axis=1, keepdims=True) for x in scores]
            raised = [jnp.exp2((x - top) * SCORE) for x, top in zip(scores, tops)]
            totals = [jnp.sum(x, axis=1, keepdims=True) for x in raised]
            probs = [(x * (1.0 / total)).astype(BF16) for x, total in zip(raised, totals)]
            for i in range(batch):
                rows = pl.ds(pl.multiple_of((s4 * batch + i) * 16, 16), 16)
                p = pltpu.roll(probs[i], 1, 1)
                att = jnp.dot(p, values[i], preferred_element_type=F32).astype(BF16)
                for h in range(HEADS):
                    ap[rows, h * HD : (h + 1) * HD] = att[h * 16 : (h + 1) * 16]
            return c

        parts = SEQ_BLOCK // batch // 2
        lax.fori_loop(half * parts, (half + 1) * parts, some, 0)
        rows = slice(half * 80, (half + 1) * 80)
        for n in range(4):
            at = slice(n * 256, (n + 1) * 256)
            padded = ap[half * 128 : (half + 1) * 128, at]
            ab[j, rows, at] = jnp.dot(
                unpad_ref[...], padded, preferred_element_type=F32
            ).astype(BF16)

    def powers(t, sign, first=0, count=ROWS_B):
        e = exps[pl.ds(pl.multiple_of(t * ROWS_B + first, 16), count), :].astype(jnp.int32)
        if sign < 0:
            return jnp.left_shift(1, -e).astype(F32)
        return jnp.left_shift(1, e + 11).astype(F32) * (2.0**-11)

    def out_project(att, weights, k, t, order, extra, done, first=0, count=ROWS_B):
        shrink = powers(t, -1, first, count)
        rows = slice(first, first + count)
        for q in order:
            for base in (q * CH, q * CH + 512):
                part = jnp.dot(att, weights[:, base : base + 512], preferred_element_type=F32)
                for g in range(4):
                    at = slice(base + g * HD, base + (g + 1) * HD)
                    group = base // HD + g
                    scaled = part[:, g * HD : (g + 1) * HD] * shrink[:, group : group + 1]
                    scaled = jnp.clip(scaled, -127.0, 127.0).astype(BF16)
                    for r in extra(q, g == 0 and base == q * CH):
                        scaled = scaled.astype(F32) + r[rows, at].astype(F32)
                    pb[k, rows, at] = scaled.astype(BF16)
            done(q)

    def column_block(j):
        return j - j // 4

    def second(k, dy, order, send_sum, half=None, part=None):
        first, count = HALVES[part] if part is not None else (0, ROWS_B)

        def extra(q, opening):
            refs = [pb.at[k]]
            if half is not None and q in half[1]:
                if opening and part == 0:
                    arrived(half[0], (half[1].index(q),))
                refs.append(rb.at[R_HALF])
            return refs

        out_project(
            bb[k, first : first + count], w_two, k, mx * 4 + (my + dy) % 4, order, extra, send_sum,
            first, count,
        )

    def near(up, part, order):
        name = "sum_up" if up else "sum_down"

        def send_sum(q):
            send(name, (part * NQ + q,))

        if up:
            second(NEAR_P, 1, order, send_sum, ("half_up", (2, 3)), part)
        else:
            second(NEAR_M, 3, order, send_sum, ("half_down", (0, 1)), part)

    def when(j, k, action):
        pl.when(j == k)(action)

    def before(j):
        @functools.partial(when, j, 1)
        def _():
            arrived("own_up", (0,))
            send("far_up", (0,))
            send("own_up", (2,))
            arrived("own_down", (2,))
            send("far_down", (0,))
            send("own_down", (0,))
            for i in range(4):
                arrived("w_beyond", (i,))
                send("w_zup", (i,))
                send("w_zdown", (i,))
                if i == 1:
                    arrived("own_up", (1,))
                    send("far_up", (1,))
                    send("own_up", (3,))
                    arrived("own_down", (3,))
                    send("far_down", (1,))
                    send("own_down", (1,))
            arrived("far_up", (0,))
            send("far_across", (0,))
            arrived("far_down", (0,))
            send("far_across", (2,))
            send("w_core0")
            arrived("own_across", (0, 1, 2))
            send("side_up", (0, 1, 2))
            send("side_down", (0, 1, 2))
            arrived("w_zup", (0, 1))
            send("w_fwd_up")
            arrived("w_zdown", (2, 3))
            send("w_fwd_down")
            arrived("far_up", (1,))
            send("far_across", (1,))
            arrived("far_down", (1,))
            send("far_across", (3,))
            send("own_across", (3,))

        @functools.partial(when, j, 2)
        def _():
            arrived("w_zup", (2, 3))
            send("w_core3")
            arrived("w_zdown", (0, 1))
            send("w_core1")
            arrived("own_up", (2, 3))

        @functools.partial(when, j, 3)
        def _():
            arrived("w_fwd_up")
            arrived("w_fwd_down")
            send("w_core2")
            arrived("far_across")

        @functools.partial(when, j, 4)
        def _():
            arrived("own_down", (0, 1))
            arrived("own_across", (3,))
            send("side_up", (3,))
            send("side_down", (3,))

        @functools.partial(when, j, 5)
        def _():
            for name in ("w_core0", "w_core3", "w_core1", "w_core2"):
                arrived(name)
            arrived("att_far")
            second(FAR, 2, (0, 2, 1, 3), lambda q: send("half_down" if q < 2 else "half_up", (q % 2,)))
            arrived("side_up", (0, 1, 2))
            arrived("side_down", (0, 1, 2))
            project_sides(True)
            arrived("side_up", (3,))
            arrived("side_down", (3,))
            project_sides(False)

        @functools.partial(when, j, 7)
        def _():
            arrived("att_near_m", (0,))
            near(False, 0, (2, 3))
            arrived("att_near_p", (0,))
            near(True, 0, (0, 1))
            near(False, 0, (0, 1))
            near(True, 0, (2, 3))
            arrived("att_near_m", (1,))
            near(False, 1, (2, 3, 0, 1))
            arrived("att_near_p", (1,))
            near(True, 1, (0, 1, 2, 3))

    def step(j, c):
        dx = (DX_BITS >> j) & 1
        dy = (DY_BITS >> (2 * j)) & 3
        t = ((mx + dx) % 2) * 4 + (my + dy) % 4
        before(j)

        @pl.when((j < 5) | (j == 7))
        def _():
            project(j)

        spread_out(j // 6 - j // 7)
        for half in range(2):
            attend(j, t, half)
            when(j, 3, functools.partial(send, "att_far", (half,)))
            when(j, 7, functools.partial(send, "att_own", (half,)))
            if half == 0:
                when(j, 5, functools.partial(send, "att_near_m", (0,)))
            when(j, 6, functools.partial(send, "att_near_p", (half,)))
            if half == 0:
                when(j, 6, functools.partial(send, "att_near_m", (1,)))

        @pl.when(dx == 0)
        def _():
            out_project(
                ab[j], w_out, column_block(j), t, range(NQ), lambda q, first: (), lambda q: None
            )

        return c

    load_q.wait()
    load_k.wait()
    load_v.wait()
    load_kv.wait()
    lax.fori_loop(0, 8, step, 0)

    arrived("att_own")
    second(OWN, 0, range(NQ), lambda q: None)

    last = ("sum_down", "sum_up")
    for name in (*ROUTES, *WEIGHTS):
        if name not in last:
            for i in pieces_of(name, None):
                route(name, i).wait_send()
    restore = powers(me, 1)
    for part in range(2):
        rows = slice(part * HALF, (part + 1) * HALF)
        for q in (0, 2, 1, 3):
            arrived("sum_down", (part * NQ + q,))
            arrived("sum_up", (part * NQ + q,))
            for g in range(CH // HD):
                group = q * (CH // HD) + g
                at = slice(group * HD, (group + 1) * HD)
                total = pb[OWN, rows, at].astype(F32)
                for r in (R_P, R_M):
                    total = total + rb[r, rows, at].astype(F32)
                mixed = raw[rows, at].astype(F32) + total * restore[rows, group : group + 1]
                raw[rows, at] = mixed.astype(BF16)
    for name in last:
        for i in pieces_of(name, None):
            route(name, i).wait_send()


def tables():
    position = (np.arange(ROWS_B) % NEW + CACHE).astype(np.float32)
    frequency = THETA ** (-(np.arange(HD // 2, dtype=np.float32) * np.float32(2.0)) / np.float32(HD))
    angles = position[:, None] * frequency.astype(np.float32)[None, :]
    cosine, sine = np.cos(angles), np.sin(angles)
    row = np.arange(ROWS_B)
    spread = np.zeros((PADDED, ROWS_B), np.float32)
    spread[row // NEW * 16 + row % NEW, row] = 1.0
    keys = np.zeros((SPREAD, ROWS_B), np.float32)
    keys[row // NEW * 32 + 2 * (row % NEW) + 1, row] = 1.0
    values = np.zeros((SPREAD, ROWS_B), np.float32)
    values[row // NEW * 32 + 2 * (row % NEW) + 2, row] = 1.0
    even = np.broadcast_to((np.arange(32) % 2 == 0)[:, None], (32, HD))
    return (
        jnp.asarray(np.concatenate([cosine, cosine], 1), F32),
        jnp.asarray(np.concatenate([-sine, sine], 1), F32),
        jnp.asarray(spread, BF16),
        jnp.asarray(spread.T[: ROWS_B // 2, : PADDED // 2], BF16),
        jnp.asarray(keys, BF16),
        jnp.asarray(values, BF16),
        jnp.asarray(np.stack([even, ~even]), BF16),
    )


def on_device(
    tokens, norm_gain, query_weight, key_weight, value_weight, out_weight, past_cache, exponents
):
    seqs = past_cache.shape[0]
    pairs = past_cache.reshape(seqs, 2 * CACHE, HD)
    anywhere = pl.BlockSpec(memory_space=pl.ANY)
    return pl.pallas_call(
        body,
        out_shape=pltpu.VMEM(tokens.shape, BF16),
        in_specs=[anywhere] * 15,
        out_specs=pl.BlockSpec(memory_space=pltpu.VMEM),
        scratch_shapes=[
            pltpu.VMEM((8, ROWS_B, D), BF16),
            pltpu.VMEM((4, ROWS_B, D), BF16),
            pltpu.VMEM((3, ROWS_B, D), BF16),
            pltpu.VMEM((8, ROWS_B, QC), BF16),
            pltpu.VMEM((4, ROWS_B, QC), BF16),
            pltpu.VMEM((D, QC + 2 * HD), BF16),
            pltpu.VMEM((QC, D), BF16),
            pltpu.VMEM((QC, D), BF16),
            pltpu.VMEM((seqs, 2 * CACHE, HD), BF16),
            pltpu.VMEM((2 * ROWS_B, QC + 2 * HD), F32),
            pltpu.VMEM((2, ROWS_B, QC + 2 * HD), BF16),
            pltpu.VMEM((PADDED, QC), BF16),
            pltpu.VMEM((SPREAD, HD), BF16),
            pltpu.VMEM((SPREAD, HD), BF16),
            pltpu.VMEM((PADDED, QC), BF16),
            pltpu.VMEM((8 * ROWS_B, HD), F32),
            pltpu.VMEM((16, D), F32),
            pltpu.VMEM((D // HD, HD), BF16),
            pltpu.VMEM((D // HD, exponents.shape[0]), jnp.int32),
            pltpu.VMEM((ROWS_B, HD), F32),
            pltpu.VMEM((ROWS_B, HD), F32),
            pltpu.VMEM((PADDED, ROWS_B), BF16),
            pltpu.VMEM((ROWS_B // 2, PADDED // 2), BF16),
            pltpu.VMEM((SPREAD, ROWS_B), BF16),
            pltpu.VMEM((SPREAD, ROWS_B), BF16),
            pltpu.VMEM((2, 32, HD), BF16),
            pltpu.SemaphoreType.DMA((15,)),
            pltpu.SemaphoreType.DMA((COUNT,)),
            pltpu.SemaphoreType.DMA((COUNT,)),
        ],
        compiler_params=pltpu.CompilerParams(
            collective_id=0, has_side_effects=True, vmem_limit_bytes=64_000_000
        ),
        name="verify_block",
    )(
        tokens, norm_gain.reshape(D // HD, HD), query_weight, key_weight, value_weight, out_weight,
        pairs, exponents.T, *tables(),
    )


def solution(mesh):
    return jax.shard_map(
        on_device,
        mesh=mesh,
        in_specs=(
            P(("dp", "tensor"), None),
            P(),
            P(None, "tensor"),
            P(None, "tensor"),
            P(None, "tensor"),
            P("tensor", None),
            P("dp", None, None, "tensor"),
            P("dp", None),
        ),
        out_specs=P(("dp", "tensor"), None),
        check_vma=False,
    )
```
